128 devices in a mesh: region: 16 (over y_lo, z, core), depth: 2 (over y_hi), member: 4 (over x).
Axes of the slice: x: 4, y: 4 (y_hi: 2, y_lo: 2; y = y_hi * 2 + y_lo), z: 4, core: 2. Of those that a mesh axis runs over, the one named last changes fastest.
Arguments:
- ensemble: bfloat16 [14, 384, 16384], P('depth', 'member', 'region'), may hold values from -6 to 6
- obs_weights: float32 [14], P('depth'), may hold values from -1.5 to 1.5
- obs_tiles: int32 [8192], P('region'), may hold values from 0 to 1023
- obs_values: float32 [8192], P('region'), may hold values from -8 to 8
- obs_error: float32 [8192], P('region'), may hold values from 0.2 to 2
- obs_noise: float32 [384, 8192], P('member', 'region'), may hold values from -6 to 6
Outputs:
- analysis: bfloat16 [14, 384, 16384], P('depth', 'member', 'region')
- inflation: float32 [], replicated
The draws below stay inside these ranges and needn't reach their ends.
Inputs may be any that keep to these rules, and one draw needn't show every extreme that they name: `obs_tiles`: the tile of the observation, counted within the 1024 tiles of the region whose block holds the observation.
All inputs are finite; a program needn't handle non-finite values.
Results may differ from the reference program's by a relative error of at most 0.011.
Values may be sent and summed in bfloat16 or wider, within the bound.
A program may use at most 64 MiB of HBM per device.

```python
import math
import jax
import jax.numpy as jnp
from jax import lax

VARS = 14
MEMBERS = 384
TILE_DEV = 1024
OBS_DEV = 512
NTILES = 16384
NOBS = 8192
RADIUS = 1024
N_REGION = 16


def touch_ends(values, own_key, smallest, largest):
    shape = values.shape
    spot = [jax.random.randint(jax.random.fold_in(own_key, axis), (), 0, shape[axis]) for axis in range(len(shape))]
    values = values.at[tuple(spot)].set(smallest)
    longest = shape.index(max(shape))
    spot[longest] = (spot[longest] + 1) % shape[longest]
    return values.at[tuple(spot)].set(largest)


def block_levels(key, dims, cuts, least, top_value):
    level = 1.0
    for dim, blocks in cuts:
        draws = jax.random.uniform(jax.random.fold_in(jax.random.fold_in(key, 6), dim), (blocks,), jnp.float32, least / len(cuts), top_value / len(cuts))
        level = level * jnp.repeat(jnp.exp(draws), dims[dim] // blocks).reshape((-1,) + (1,) * (len(dims) - 1 - dim))
    return level


def gaussian(key, dims, scale, limit, split=(), kind=jnp.bfloat16):
    factor_of = block_levels(key, dims, split, -0.22, 0.18) if split else 1.0
    drawn = jax.random.normal(key, dims, jnp.float32) * scale * factor_of
    return jnp.minimum(jnp.maximum(drawn, -limit), limit).astype(kind)


def setup_inputs(seed: int = 0) -> dict:
    splits = jax.random.split(jax.random.key(seed), 7)
    return {
        "ensemble": gaussian(splits[0], (VARS, MEMBERS, NTILES), 1.0, 6.0, ((0, 2), (1, 4), (2, 16))),
        "obs_weights": gaussian(splits[1], (VARS,), VARS ** -0.5, 1.5, ((0, 2),), jnp.float32),
        "obs_tiles": touch_ends(jax.random.randint(splits[2], (NOBS,), 0, TILE_DEV), jax.random.fold_in(splits[2], 1), 0, TILE_DEV - 1).astype(jnp.int32),
        "obs_values": gaussian(splits[3], (NOBS,), 2.0, 8.0, ((0, 16),), jnp.float32),
        "obs_error": jnp.clip(jnp.exp(math.log(2.0) - 2.3025851 * jax.random.uniform(splits[4], (NOBS,), jnp.float32) ** block_levels(splits[4], (NOBS,), ((0, 16),), -0.2, 0.2)), 0.2, 2.0),
        "obs_noise": gaussian(splits[5], (MEMBERS, NOBS), 1.0, 6.0, ((0, 4), (1, 16)), jnp.float32),
    }


def reference(ensemble, obs_weights, obs_tiles, obs_values, obs_error, obs_noise):
    state_f = ensemble.astype(jnp.float32)
    state_mean = lax.optimization_barrier(jnp.sum(state_f, axis=1)) / MEMBERS
    anomalies = (state_f - state_mean[:, None, :]).astype(jnp.bfloat16)
    obs_region = jnp.arange(NOBS, dtype=jnp.int32) // OBS_DEV
    obs_global = obs_region * TILE_DEV + obs_tiles.astype(jnp.int32)
    picked = jnp.take(ensemble, obs_global, axis=2).astype(jnp.float32)
    predicted = jnp.einsum('lmk,l->mk', picked, obs_weights.astype(jnp.float32), precision=lax.Precision.HIGHEST)
    obs_mean = lax.optimization_barrier(jnp.sum(predicted, axis=0)) / MEMBERS
    obs_dev = predicted - obs_mean[None, :]
    obs_spread = lax.optimization_barrier(jnp.sum(obs_dev * obs_dev, axis=0)) / (MEMBERS - 1)
    innovation = obs_values - obs_mean
    inflation = jnp.sum(innovation * innovation) / jnp.sum(obs_spread + obs_error)
    infl_root = jnp.sqrt(inflation)
    factor = inflation / (inflation * obs_spread + obs_error)
    obs_anom = obs_dev.astype(jnp.bfloat16)
    perturbed = (innovation[None, :] + jnp.sqrt(obs_error)[None, :] * obs_noise - infl_root * obs_dev).astype(jnp.bfloat16)
    padded_anom = jnp.pad(obs_anom, ((0, 0), (OBS_DEV, OBS_DEV)))
    padded_pert = jnp.pad(perturbed, ((0, 0), (OBS_DEV, OBS_DEV)))
    padded_factor = jnp.pad(factor, (OBS_DEV, OBS_DEV))
    padded_pos = jnp.pad(obs_global.astype(jnp.float32), (OBS_DEV, OBS_DEV))

    def one_region(region_id):
        first_obs = region_id * OBS_DEV
        anom_window = lax.dynamic_slice_in_dim(padded_anom, first_obs, 3 * OBS_DEV, 1).astype(jnp.float32)
        pert_window = lax.dynamic_slice_in_dim(padded_pert, first_obs, 3 * OBS_DEV, 1).astype(jnp.float32)
        factor_window = lax.dynamic_slice_in_dim(padded_factor, first_obs, 3 * OBS_DEV, 0)
        pos_window = lax.dynamic_slice_in_dim(padded_pos, first_obs, 3 * OBS_DEV, 0)
        first_tile = region_id * TILE_DEV
        region_anom = lax.dynamic_slice_in_dim(anomalies, first_tile, TILE_DEV, 2).astype(jnp.float32)
        region_mean = lax.dynamic_slice_in_dim(state_mean, first_tile, TILE_DEV, 1)
        covariance = jnp.einsum('lmt,mj->ltj', region_anom, anom_window) / (MEMBERS - 1)
        tile_pos = (first_tile + jnp.arange(TILE_DEV, dtype=jnp.int32)).astype(jnp.float32)
        closeness = jnp.maximum(0.0, 1.0 - jnp.abs(tile_pos[:, None] - pos_window[None, :]) / RADIUS)
        kalman_gain = (covariance * (closeness * closeness * factor_window[None, :])[None]).astype(jnp.bfloat16)
        increment = jnp.einsum('ltj,mj->lmt', kalman_gain.astype(jnp.float32), pert_window)
        return (region_mean[:, None, :] + infl_root * region_anom + increment).astype(jnp.bfloat16)
    region_out = lax.map(one_region, jnp.arange(N_REGION, dtype=jnp.int32))
    analysis = jnp.transpose(region_out, (1, 2, 0, 3)).reshape(VARS, MEMBERS, NTILES)
    return (analysis, inflation)
```

```python
import jax
import jax.numpy as jnp
from jax import lax
from jax.experimental import pallas as pl
from jax.experimental.pallas import tpu as pltpu
from jax.sharding import PartitionSpec as P

MEMBERS = 384
RADIUS = 1024.0
MESH = pl.DeviceIdType.MESH
F32 = jnp.float32
BF16 = jnp.bfloat16


def dot(a, b):
    return lax.dot_general(a, b, (((1,), (0,)), ((), ())), preferred_element_type=F32)


def kernel(
    regions,
    peers,
    ens_hbm,
    wts_hbm,
    tiles_hbm,
    vals_hbm,
    err_hbm,
    noise_hbm,
    out_hbm,
    infl_ref,
    ens,
    wts,
    small,
    noise,
    blend,
    hot,
    part,
    obs,
    slots,
    recv,
    hold,
    back,
    back_hold,
    anom_t,
    taper,
    gain,
    pert,
    tot,
    load_sem,
    e_send,
    e_recv,
    b_send,
    b_recv,
    o_send,
    o_recv,
    n_send,
    n_recv,
    s_send,
    s_recv,
    d_send,
    d_recv,
    i_send,
    i_recv,
    own_sem,
    out_sem,
):
    n_var, own, n_tile = ens.shape
    n_obs = noise.shape[1]
    half = own // 2
    share = n_tile // peers
    r = lax.axis_index("region")
    d = lax.axis_index("depth")
    j = lax.axis_index("member")
    right, left, opp = lax.rem(j + 1, peers), lax.rem(j + 3, peers), lax.rem(j + 2, peers)
    after, before = lax.rem(r + 1, regions), lax.rem(r + regions - 1, regions)

    def rows(b, start=0, count=None):
        return pl.ds(pl.multiple_of(b * own + start, 16), own if count is None else count)

    def cols(b):
        return pl.ds(pl.multiple_of(b * share, 128), share)

    def remote(src, dst, send, rec, **where):
        return pltpu.make_async_remote_copy(src, dst, send, rec, device_id=where, device_id_type=MESH)

    loads = [
        pltpu.make_async_copy(noise_hbm, noise, load_sem.at[0]),
        pltpu.make_async_copy(err_hbm, small.at[1, pl.ds(2, 1)], load_sem.at[1]),
        pltpu.make_async_copy(tiles_hbm, small.at[1, pl.ds(0, 1)], load_sem.at[2]),
        pltpu.make_async_copy(vals_hbm, small.at[1, pl.ds(1, 1)], load_sem.at[3]),
        pltpu.make_async_copy(wts_hbm, wts, load_sem.at[4]),
        pltpu.make_async_copy(ens_hbm, ens, load_sem.at[5]),
    ]
    for copy in loads:
        copy.start()

    def take_own(l):
        return pltpu.make_async_copy(ens_hbm.at[l, :, cols(j)], recv.at[l, rows(j), :], own_sem.at[l])

    lax.fori_loop(0, n_var, lambda l, c: (take_own(l).start(), c)[1], 0)

    barrier = pltpu.get_barrier_semaphore()
    pl.semaphore_signal(barrier, inc=1, device_id={"member": right}, device_id_type=MESH)
    pl.semaphore_signal(barrier, inc=1, device_id={"member": left}, device_id_type=MESH)
    pl.semaphore_signal(barrier, inc=1, device_id={"depth": 1 - d}, device_id_type=MESH)

    def greet(o, c):
        pl.semaphore_signal(barrier, inc=1, device_id={"region": lax.rem(r + o, regions)}, device_id_type=MESH)
        return c

    lax.fori_loop(1, regions, greet, 0)

    for copy in loads[:4]:
        copy.wait()
    obs[1, 0, rows(j), :] = (jnp.sqrt(small[1, 2:3, :]) * noise[...]).astype(BF16)
    loads[4].wait()
    loads[5].wait()
    pl.semaphore_wait(barrier, regions + 2)

    def e_copies(l):
        return (
            remote(ens.at[l, pl.ds(0, half), cols(opp)], hold.at[0, l], e_send.at[2], e_recv.at[2, l], member=right),
            remote(ens.at[l, pl.ds(half, half), cols(opp)], hold.at[1, l], e_send.at[3], e_recv.at[3, l], member=left),
            remote(ens.at[l, :, cols(right)], recv.at[l, rows(j), :], e_send.at[0], e_recv.at[0, l], member=right),
            remote(ens.at[l, :, cols(left)], recv.at[l, rows(j), :], e_send.at[1], e_recv.at[1, l], member=left),
        )

    def e_relays(l):
        return (
            remote(hold.at[0, l], recv.at[l, rows(left, 0, half), :], e_send.at[4], e_recv.at[4, l], member=right),
            remote(hold.at[1, l], recv.at[l, rows(right, half, half), :], e_send.at[5], e_recv.at[5, l], member=left),
        )

    def send_ens(first, last):
        def body(l, c):
            for copy in e_copies(l):
                copy.start()
            return c

        lax.fori_loop(first, last, body, 0)

    def relay_ens(l):
        held, fwd = e_copies(l), e_relays(l)
        held[0].wait_recv()
        fwd[0].start()
        held[1].wait_recv()
        fwd[1].start()

    def take_ens(l):
        copies, fwd = e_copies(l), e_relays(l)
        take_own(l).wait()
        copies[2].wait_recv()
        copies[3].wait_recv()
        fwd[0].wait_recv()
        fwd[1].wait_recv()

    def o_copies(q):
        block = obs.at[1, q, rows(j), :]
        return (
            remote(block, block, o_send.at[q, 0], o_recv.at[q, 0], member=right),
            remote(block, block, o_send.at[q, 1], o_recv.at[q, 1], member=left),
        )

    def o_relays(q):
        top, low = obs.at[1, q, rows(left, 0, half), :], obs.at[1, q, rows(right, half, half), :]
        return (
            remote(top, top, o_send.at[q, 2], o_recv.at[q, 2], member=right),
            remote(low, low, o_send.at[q, 3], o_recv.at[q, 3], member=left),
        )

    def to_beside(q, b):
        block = obs.at[1, q, rows(b), :]
        remote(block, obs.at[0, q, rows(b), :], n_send.at[q, 0], n_recv.at[q, 0], region=after).start()
        remote(block, obs.at[2, q, rows(b), :], n_send.at[q, 1], n_recv.at[q, 1], region=before).start()

    def from_beside(q):
        return (
            remote(obs.at[1, q], obs.at[0, q], n_send.at[q, 0], n_recv.at[q, 0], region=after),
            remote(obs.at[1, q], obs.at[2, q], n_send.at[q, 1], n_recv.at[q, 1], region=before),
        )

    small_copies = (
        remote(small.at[1], small.at[0], s_send.at[0], s_recv.at[0], region=after),
        remote(small.at[1], small.at[2], s_send.at[1], s_recv.at[1], region=before),
    )

    def spread_block(q, relay):
        for k, copy in enumerate(o_copies(q)):
            copy.wait_recv()
            o_relays(q)[k].start()
        to_beside(q, left)
        to_beside(q, right)

    def finish_block(q):
        for copy in o_relays(q):
            copy.wait_recv()
        to_beside(q, opp)

    send_ens(0, 3)
    for copy in small_copies:
        copy.start()
    to_beside(0, j)
    for copy in o_copies(0):
        copy.start()

    def blended(i, c):
        at = pl.ds(pl.multiple_of(i * 16, 16), 16)
        total = wts[0] * ens[0, at, :].astype(F32)
        for l in range(1, n_var):
            total = total + wts[l] * ens[l, at, :].astype(F32)
        blend[at, :] = total.astype(BF16)
        return c

    lax.fori_loop(0, own // 16, blended, 0)
    tile_row = small[1, 0:1, :]

    def one_hot(i, c):
        at = pl.ds(pl.multiple_of(i * 128, 128), 128)
        index = (lax.broadcasted_iota(jnp.int32, (128, n_obs), 0) + i * 128).astype(F32)
        hot[at, :] = jnp.where(index == tile_row, 1.0, 0.0).astype(BF16)
        return c

    lax.fori_loop(0, n_tile // 128, one_hot, 0)
    part[0] = dot(blend[...], hot[...]).astype(BF16)
    swap = remote(part.at[0], part.at[1], d_send, d_recv, depth=1 - d)
    swap.start()

    relay_ens(0)
    relay_ens(1)
    swap.wait_recv()
    obs[1, 1, rows(j), :] = (part[0].astype(F32) + part[1].astype(F32)).astype(BF16)
    for copy in o_copies(1):
        copy.start()
    to_beside(1, j)
    send_ens(3, 4)
    relay_ens(2)
    spread_block(0, None)
    spread_block(1, None)
    send_ens(4, 7)
    finish_block(0)
    relay_ens(3)
    finish_block(1)

    def stats(w):
        pred = obs[w, 1].astype(F32)
        mean = jnp.sum(pred, axis=0, keepdims=True) / MEMBERS
        dev = pred - mean
        spread = jnp.sum(dev * dev, axis=0, keepdims=True) / (MEMBERS - 1)
        tot[w, 0:1, :] = mean
        tot[w, 1:2, :] = spread
        anom_t[pl.ds(w * n_obs, n_obs), :] = dev.T.astype(BF16)
        return small[w, 1:2, :] - mean, spread

    innovation, spread = stats(1)
    squares = jnp.sum(innovation * innovation, axis=1, keepdims=True)
    widths = jnp.sum(spread + small[1, 2:3, :], axis=1, keepdims=True)
    line = lax.broadcasted_iota(jnp.int32, (8, 128), 0)
    slots[r] = jnp.where(line < 4, squares, widths)

    def tell(o, c):
        remote(slots.at[r], slots.at[r], i_send, i_recv, region=lax.rem(r + o, regions)).start()
        return c

    lax.fori_loop(1, regions, tell, 0)

    for copy in small_copies:
        copy.wait_recv()
    lane = lax.broadcasted_iota(jnp.int32, (n_obs, 128), 1) + j * share
    shifts = (
        jnp.where(r == 0, -16.0 * RADIUS, -RADIUS),
        jnp.float32(0.0),
        jnp.where(r == regions - 1, 16.0 * RADIUS, RADIUS),
    )
    for w in range(3):
        spot = jnp.broadcast_to(small[w, 0:1, :] + shifts[w], (128, n_obs)).T
        for c in range(share // 128):
            near = jnp.maximum(0.0, 1.0 - jnp.abs((lane + c * 128).astype(F32) - spot) / RADIUS)
            taper[pl.ds(w * n_obs, n_obs), pl.ds(c * 128, 128)] = near * near / (MEMBERS - 1)

    relay_ens(4)
    for q in range(2):
        for copy in from_beside(q):
            copy.wait_recv()
    stats(0)
    stats(2)

    remote(slots.at[pl.ds(0, regions - 1)], slots.at[pl.ds(1, regions - 1)], i_send, i_recv, region=after).wait_recv()
    total = jnp.sum(slots[...], axis=0)
    infl = total[0:1, 0:1] / total[4:5, 0:1]
    root = jnp.sqrt(infl)
    infl_ref[0, 0] = infl[0, 0]

    for w in range(3):
        mean, spread = tot[w, 0:1, :], tot[w, 1:2, :]
        factor = infl / (infl * spread + small[w, 2:3, :])
        innovation = small[w, 1:2, :] - mean
        dev = obs[w, 1].astype(F32) - mean
        moved = innovation + obs[w, 0].astype(F32) - root * dev
        pert[:, pl.ds(w * n_obs, n_obs)] = (moved * factor).astype(BF16)

    def b_copies(l):
        return (
            remote(back.at[l, rows(opp, 0, half), :], back_hold.at[0, l], b_send.at[2], b_recv.at[2, l], member=right),
            remote(back.at[l, rows(opp, half, half), :], back_hold.at[1, l], b_send.at[3], b_recv.at[3, l], member=left),
            remote(back.at[l, rows(right), :], out_hbm.at[l, :, cols(j)], b_send.at[0], b_recv.at[0, l], member=right),
            remote(back.at[l, rows(left), :], out_hbm.at[l, :, cols(j)], b_send.at[1], b_recv.at[1, l], member=left),
        )

    def b_relays(l):
        return (
            remote(back_hold.at[0, l], out_hbm.at[l, pl.ds(0, half), cols(left)], b_send.at[4], b_recv.at[4, l], member=right),
            remote(back_hold.at[1, l], out_hbm.at[l, pl.ds(half, half), cols(right)], b_send.at[5], b_recv.at[5, l], member=left),
        )

    def keep(l):
        return pltpu.make_async_copy(back.at[l, rows(j), :], out_hbm.at[l, :, cols(j)], out_sem.at[l])

    def relay_back(l):
        held, fwd = b_copies(l), b_relays(l)
        held[0].wait_recv()
        fwd[0].start()
        held[1].wait_recv()
        fwd[1].start()

    def analyse(l, c):
        @pl.when(l < 2)
        def _():
            relay_ens(l + 5)

        take_ens(l)
        state = recv[l].astype(F32)
        mean = jnp.sum(state, axis=0, keepdims=True) / MEMBERS
        anom = (state - mean).astype(BF16)
        for w in range(3):
            at = pl.ds(w * n_obs, n_obs)
            gain[at, :] = (dot(anom_t[at, :], anom) * taper[at, :]).astype(BF16)
        increment = dot(pert[...], gain[...])
        back[l] = (mean + root * anom.astype(F32) + increment).astype(BF16)
        for copy in b_copies(l):
            copy.start()
        keep(l).start()

        @pl.when(l > 0)
        def _():
            relay_back(l - 1)

        return c

    lax.fori_loop(0, n_var, analyse, 0)
    relay_back(n_var - 1)

    def finish(l, c):
        copies, fwd = b_copies(l), b_relays(l)
        keep(l).wait()
        copies[2].wait_recv()
        copies[3].wait_recv()
        fwd[0].wait_recv()
        fwd[1].wait_recv()
        return c

    lax.fori_loop(0, n_var, finish, 0)

    whole, part_of = recv.at[:, pl.ds(0, own), :], hold.at[0]
    for sems in (e_send, b_send):
        for k in range(6):
            block = whole if k < 2 else part_of
            remote(block, block, sems.at[k], e_recv.at[0, 0], member=right).wait_send()
    for q in range(2):
        for copy in o_copies(q) + o_relays(q) + from_beside(q):
            copy.wait_send()
    for copy in small_copies:
        copy.wait_send()
    swap.wait_send()
    remote(slots.at[pl.ds(0, regions - 1)], slots.at[pl.ds(1, regions - 1)], i_send, i_recv, region=after).wait_send()


def solution(mesh):
    regions, peers = mesh.shape["region"], mesh.shape["member"]

    def shards(ensemble, obs_weights, obs_tiles, obs_values, obs_error, obs_noise):
        n_var, own, n_tile = ensemble.shape
        n_obs = obs_tiles.shape[0]
        share, members = n_tile // peers, own * peers
        DMA = pltpu.SemaphoreType.DMA
        scratch = [
            pltpu.VMEM((n_var, own, n_tile), BF16),
            pltpu.SMEM((n_var,), F32),
            pltpu.VMEM((3, 8, n_obs), F32),
            pltpu.VMEM((own, n_obs), F32),
            pltpu.VMEM((own, n_tile), BF16),
            pltpu.VMEM((n_tile, n_obs), BF16),
            pltpu.VMEM((2, own, n_obs), BF16),
            pltpu.VMEM((3, 2, members, n_obs), BF16),
            pltpu.VMEM((regions, 8, 128), F32),
            pltpu.VMEM((n_var, members, share), BF16),
            pltpu.VMEM((2, n_var, own // 2, share), BF16),
            pltpu.VMEM((n_var, members, share), BF16),
            pltpu.VMEM((2, n_var, own // 2, share), BF16),
            pltpu.VMEM((3 * n_obs, members), BF16),
            pltpu.VMEM((3 * n_obs, share), F32),
            pltpu.VMEM((3 * n_obs, share), BF16),
            pltpu.VMEM((members, 3 * n_obs), BF16),
            pltpu.VMEM((3, 8, n_obs), F32),
            DMA((6,)),
            DMA((6,)),
            DMA((6, n_var)),
            DMA((6,)),
            DMA((6, n_var)),
            DMA((2, 4)),
            DMA((2, 4)),
            DMA((2, 2)),
            DMA((2, 2)),
            DMA((2,)),
            DMA((2,)),
            DMA,
            DMA,
            DMA,
            DMA,
            DMA((n_var,)),
            DMA((n_var,)),
        ]
        hbm = pl.BlockSpec(memory_space=pl.ANY)
        analysis, inflation = pl.pallas_call(
            lambda *refs: kernel(regions, peers, *refs),
            out_shape=(
                jax.ShapeDtypeStruct(ensemble.shape, BF16),
                jax.ShapeDtypeStruct((1, 1), F32),
            ),
            in_specs=[hbm] * 6,
            out_specs=(hbm, pl.BlockSpec(memory_space=pltpu.SMEM)),
            scratch_shapes=scratch,
            compiler_params=pltpu.CompilerParams(
                collective_id=0, has_side_effects=True, vmem_limit_bytes=56 * 2**20
            ),
        )(
            ensemble,
            obs_weights,
            obs_tiles.astype(F32).reshape(1, n_obs),
            obs_values.reshape(1, n_obs),
            obs_error.reshape(1, n_obs),
            obs_noise,
        )
        return analysis, inflation.reshape(())

    return jax.shard_map(
        shards,
        mesh=mesh,
        in_specs=(
            P("depth", "member", "region"),
            P("depth"),
            P("region"),
            P("region"),
            P("region"),
            P("member", "region"),
        ),
        out_specs=(P("depth", "member", "region"), P()),
        check_vma=False,
    )
```

```python
import jax
import jax.numpy as jnp
from jax import lax
from jax.experimental import pallas as pl
from jax.experimental.pallas import tpu as pltpu
from jax.sharding import PartitionSpec as P

MEMBERS = 384
RADIUS = 1024.0
MESH = pl.DeviceIdType.MESH
F32 = jnp.float32
BF16 = jnp.bfloat16


def dot(a, b):
    return lax.dot_general(a, b, (((1,), (0,)), ((), ())), preferred_element_type=F32)


def kernel(
    regions,
    peers,
    ens_hbm,
    wts_hbm,
    tiles_hbm,
    vals_hbm,
    err_hbm,
    noise_hbm,
    out,
    infl_ref,
    ens,
    wts,
    spots,
    small,
    noise,
    blend,
    hot,
    part,
    obs,
    slots,
    recv,
    back,
    anoms,
    means,
    anom_t,
    taper,
    gain,
    pert,
    tot,
    load_sem,
    e_send,
    e_recv,
    b_send,
    b_recv,
    o_send,
    o_recv,
    y_send,
    y_recv,
    n_send,
    n_recv,
    s_send,
    s_recv,
    d_send,
    d_recv,
    i_send,
    i_recv,
    own_sem,
):
    n_var, own, n_tile = ens.shape
    n_obs = noise.shape[1]
    share = n_tile // peers
    r = lax.axis_index("region")
    d = lax.axis_index("depth")
    j = lax.axis_index("member")
    right, left, opp = lax.rem(j + 1, peers), lax.rem(j + 3, peers), lax.rem(j + 2, peers)
    after, before = lax.rem(r + 1, regions), lax.rem(r + regions - 1, regions)
    others = (opp, right, left)

    def rows(b):
        return pl.ds(pl.multiple_of(b * own, 16), own)

    def cols(b):
        return pl.ds(pl.multiple_of(b * share, 128), share)

    def half(h):
        return pl.ds(pl.multiple_of(h * (n_obs // 2), 128), n_obs // 2)

    def remote(src, dst, send, rec, **where):
        return pltpu.make_async_remote_copy(src, dst, send, rec, device_id=where, device_id_type=MESH)

    barrier = pltpu.get_barrier_semaphore()

    def greet(**where):
        pl.semaphore_signal(barrier, inc=1, device_id=where, device_id_type=MESH)

    def greet_region(o, c):
        greet(region=lax.rem(r + o, regions))
        return c

    lax.fori_loop(1, regions, greet_region, 0)
    for p in others:
        greet(member=p)
    greet(depth=1 - d)

    loads = [
        pltpu.make_async_copy(ens_hbm, ens, load_sem.at[0]),
        pltpu.make_async_copy(wts_hbm, wts, load_sem.at[1]),
        pltpu.make_async_copy(tiles_hbm, spots, load_sem.at[2]),
        pltpu.make_async_copy(err_hbm, small.at[1, pl.ds(2, 1)], load_sem.at[3]),
        pltpu.make_async_copy(vals_hbm, small.at[1, pl.ds(1, 1)], load_sem.at[4]),
        pltpu.make_async_copy(noise_hbm, noise, load_sem.at[5]),
    ]
    for copy in loads:
        copy.start()

    def take_own(l):
        return pltpu.make_async_copy(ens_hbm.at[l, :, cols(j)], recv.at[l, rows(j), :], own_sem.at[l])

    lax.fori_loop(0, n_var, lambda l, c: (take_own(l).start(), c)[1], 0)

    def blended(i, c):
        at = pl.ds(pl.multiple_of(i * 16, 16), 16)
        total = wts[0] * ens[0, at, :].astype(F32)
        for l in range(1, n_var):
            total = total + wts[l] * ens[l, at, :].astype(F32)
        blend[at, :] = total.astype(BF16)
        return c

    with jax.named_scope("load_small"):
        loads[1].wait()
        loads[2].wait()
    tile_row = spots[...].astype(F32)
    small[1, 0:1, :] = tile_row

    def one_hot(i, c):
        at = pl.ds(pl.multiple_of(i * 128, 128), 128)
        index = (lax.broadcasted_iota(jnp.int32, (128, n_obs), 0) + i * 128).astype(F32)
        hot[at, :] = jnp.where(index == tile_row, 1.0, 0.0).astype(BF16)
        return c

    with jax.named_scope("hot"):
        lax.fori_loop(0, n_tile // 128, one_hot, 0)
    with jax.named_scope("noise"):
        for copy in loads[3:]:
            copy.wait()
        obs[1, 0, rows(j), :] = (jnp.sqrt(small[1, 2:3, :]) * noise[...]).astype(BF16)
    with jax.named_scope("blend"):
        loads[0].wait()
        lax.fori_loop(0, own // 16, blended, 0)
    with jax.named_scope("pick"):
        part[0] = dot(blend[...], hot[...]).astype(BF16)
    with jax.named_scope("barrier"):
        pl.semaphore_wait(barrier, regions + 3)

    def e_copies(l):
        return [
            remote(ens.at[l, :, cols(p)], recv.at[l, rows(j), :], e_send.at[k], e_recv.at[k, l], member=p)
            for k, p in enumerate(others)
        ]

    def send_ens(first, last):
        def body(l, c):
            for copy in e_copies(l):
                copy.start()
            return c

        lax.fori_loop(first, last, body, 0)

    def o_copies(q):
        block = obs.at[1, 1, rows(j), :] if q else obs.at[1, 0, rows(j), half(d)]
        return [
            remote(block, block, o_send.at[q, k], o_recv.at[q, k], member=p) for k, p in enumerate(others)
        ]

    def to_beside(q, b, h=None):
        at = (rows(b), slice(None)) if h is None else (rows(b), half(h))
        remote(obs.at[(1, q) + at], obs.at[(0, q) + at], n_send.at[q, 0], n_recv.at[q, 0], region=after).start()
        remote(obs.at[(1, q) + at], obs.at[(2, q) + at], n_send.at[q, 1], n_recv.at[q, 1], region=before).start()

    def from_beside(q):
        return (
            remote(obs.at[1, q], obs.at[0, q], n_send.at[q, 0], n_recv.at[q, 0], region=after),
            remote(obs.at[1, q], obs.at[2, q], n_send.at[q, 1], n_recv.at[q, 1], region=before),
        )

    def to_depth(b):
        block = obs.at[1, 0, rows(b), half(d)]
        remote(block, block, y_send, y_recv, depth=1 - d).start()

    three = obs.at[1, 0, pl.ds(0, 3 * own), half(d)]
    from_depth = remote(three, three, y_send, y_recv, depth=1 - d)
    small_copies = (
        remote(small.at[1], small.at[0], s_send.at[0], s_recv.at[0], region=after),
        remote(small.at[1], small.at[2], s_send.at[1], s_recv.at[1], region=before),
    )
    swap = remote(part.at[0], part.at[1], d_send, d_recv, depth=1 - d)

    swap.start()
    for copy in o_copies(0):
        copy.start()
    send_ens(0, 1)
    for copy in small_copies:
        copy.start()
    to_beside(0, j)

    with jax.named_scope("small"):
        for copy in small_copies:
            copy.wait_recv()
    lane = lax.broadcasted_iota(jnp.int32, (n_obs, 128), 1) + j * share
    shifts = (
        jnp.where(r == 0, -16.0 * RADIUS, -RADIUS),
        jnp.float32(0.0),
        jnp.where(r == regions - 1, 16.0 * RADIUS, RADIUS),
    )
    with jax.named_scope("taper"):
        for w in range(3):
            spot = jnp.broadcast_to(small[w, 0:1, :] + shifts[w], (128, n_obs)).T
            for c in range(share // 128):
                near = jnp.maximum(0.0, 1.0 - jnp.abs((lane + c * 128).astype(F32) - spot) / RADIUS)
                taper[pl.ds(w * n_obs, n_obs), pl.ds(c * 128, 128)] = near * near / (MEMBERS - 1)

    with jax.named_scope("swap"):
        swap.wait_recv()
    obs[1, 1, rows(j), :] = (part[0].astype(F32) + part[1].astype(F32)).astype(BF16)
    for copy in o_copies(1):
        copy.start()
    to_beside(1, j)
    send_ens(1, n_var)
    with jax.named_scope("noise_x"):
        for copy, b in zip(o_copies(0), (opp, left, right)):
            copy.wait_recv()
            to_depth(b)
            to_beside(0, b, d)
    with jax.named_scope("noise_y"):
        from_depth.wait_recv()
    for b in others:
        to_beside(0, b, 1 - d)
    with jax.named_scope("pred_x"):
        for k, b in ((2, right), (1, left), (0, opp)):
            o_copies(1)[k].wait_recv()
            to_beside(1, b)

    def stats(w):
        pred = obs[w, 1].astype(F32)
        mean = jnp.sum(pred, axis=0, keepdims=True) / MEMBERS
        dev = pred - mean
        spread = jnp.sum(dev * dev, axis=0, keepdims=True) / (MEMBERS - 1)
        tot[w, 0:1, :] = mean
        tot[w, 1:2, :] = spread
        anom_t[pl.ds(w * n_obs, n_obs), :] = dev.T.astype(BF16)
        return small[w, 1:2, :] - mean, spread

    with jax.named_scope("stats1"):
        innovation, spread = stats(1)
        squares = jnp.sum(innovation * innovation, axis=1, keepdims=True)
        widths = jnp.sum(spread + small[1, 2:3, :], axis=1, keepdims=True)
        line = lax.broadcasted_iota(jnp.int32, (8, 128), 0)
        slots[r] = jnp.where(line < 4, squares, widths)

    def tell(o, c):
        remote(slots.at[r], slots.at[r], i_send, i_recv, region=lax.rem(r + o, regions)).start()
        return c

    lax.fori_loop(1, regions, tell, 0)
    told = slots.at[pl.ds(0, regions - 1)]
    tells = remote(told, told, i_send, i_recv, region=after)

    def gain_of(l, slot):
        with jax.named_scope("take"):
            take_own(l).wait()
            for copy in e_copies(l):
                copy.wait_recv()
        state = recv[l].astype(F32)
        mean = jnp.sum(state, axis=0, keepdims=True) / MEMBERS
        anom = (state - mean).astype(BF16)
        means[slot, 0:1, :] = mean
        anoms[slot] = anom
        for w in range(3):
            at = pl.ds(w * n_obs, n_obs)
            gain[slot, at, :] = (dot(anom_t[at, :], anom) * taper[at, :]).astype(BF16)

    with jax.named_scope("beside1"):
        for copy in from_beside(1):
            copy.wait_recv()
    with jax.named_scope("stats02"):
        stats(0)
        stats(2)
    with jax.named_scope("gain0"):
        gain_of(0, 0)
    with jax.named_scope("beside0"):
        for copy in from_beside(0):
            copy.wait_recv()
    with jax.named_scope("infl"):
        tells.wait_recv()
    total = jnp.sum(slots[...], axis=0)
    infl = total[0:1, 0:1] / total[4:5, 0:1]
    root = jnp.sqrt(infl)
    infl_ref[0, 0] = infl[0, 0]

    with jax.named_scope("pert"):
        for w in range(3):
            mean, spread = tot[w, 0:1, :], tot[w, 1:2, :]
            factor = infl / (infl * spread + small[w, 2:3, :])
            innovation = small[w, 1:2, :] - mean
            dev = obs[w, 1].astype(F32) - mean
            moved = innovation + obs[w, 0].astype(F32) - root * dev
            pert[:, pl.ds(w * n_obs, n_obs)] = (moved * factor).astype(BF16)

    def b_copies(l):
        return [
            remote(back.at[l, rows(p), :], out.at[l, :, cols(j)], b_send.at[k], b_recv.at[k, l], member=p)
            for k, p in enumerate(others)
        ]

    def analyse(l, c):
        slot = lax.rem(l, 2)
        with jax.named_scope("inc"):
            increment = dot(pert[...], gain[slot])
            back[l] = (means[slot, 0:1, :] + root * anoms[slot].astype(F32) + increment).astype(BF16)
        for copy in b_copies(l):
            copy.start()
        out[l, :, cols(j)] = back[l, rows(j), :]

        @pl.when(l < n_var - 1)
        def _():
            with jax.named_scope("gain"):
                gain_of(l + 1, 1 - slot)

        return c

    lax.fori_loop(0, n_var, analyse, 0)

    def finish(l, c):
        with jax.named_scope("fin"):
            for copy in b_copies(l):
                copy.wait_recv()
        return c

    lax.fori_loop(0, n_var, finish, 0)

    with jax.named_scope("sent"):
        whole = recv.at[:, pl.ds(0, own), :]
        for sems in (e_send, b_send):
            for k, p in enumerate(others):
                remote(whole, whole, sems.at[k], e_recv.at[0, 0], member=p).wait_send()
        for q in range(2):
            for copy in o_copies(q):
                copy.wait_send()
            for copy in from_beside(q):
                copy.wait_send()
        from_depth.wait_send()
        for copy in small_copies:
            copy.wait_send()
        swap.wait_send()
        tells.wait_send()


def solution(mesh):
    regions, peers = mesh.shape["region"], mesh.shape["member"]

    def shards(ensemble, obs_weights, obs_tiles, obs_values, obs_error, obs_noise):
        n_var, own, n_tile = ensemble.shape
        n_obs = obs_tiles.shape[0]
        share, members = n_tile // peers, own * peers
        DMA = pltpu.SemaphoreType.DMA
        scratch = [
            pltpu.VMEM((n_var, own, n_tile), BF16),
            pltpu.SMEM((n_var,), F32),
            pltpu.VMEM((1, n_obs), jnp.int32),
            pltpu.VMEM((3, 8, n_obs), F32),
            pltpu.VMEM((own, n_obs), F32),
            pltpu.VMEM((own, n_tile), BF16),
            pltpu.VMEM((n_tile, n_obs), BF16),
            pltpu.VMEM((2, own, n_obs), BF16),
            pltpu.VMEM((3, 2, members, n_obs), BF16),
            pltpu.VMEM((regions, 8, 128), F32),
            pltpu.VMEM((n_var, members, share), BF16),
            pltpu.VMEM((n_var, members, share), BF16),
            pltpu.VMEM((2, members, share), BF16),
            pltpu.VMEM((2, 8, share), F32),
            pltpu.VMEM((3 * n_obs, members), BF16),
            pltpu.VMEM((3 * n_obs, share), F32),
            pltpu.VMEM((2, 3 * n_obs, share), BF16),
            pltpu.VMEM((members, 3 * n_obs), BF16),
            pltpu.VMEM((3, 8, n_obs), F32),
            DMA((6,)),
            DMA((3,)),
            DMA((3, n_var)),
            DMA((3,)),
            DMA((3, n_var)),
            DMA((2, 3)),
            DMA((2, 3)),
            DMA,
            DMA,
            DMA((2, 2)),
            DMA((2, 2)),
            DMA((2,)),
            DMA((2,)),
            DMA,
            DMA,
            DMA,
            DMA,
            DMA((n_var,)),
        ]
        hbm = pl.BlockSpec(memory_space=pltpu.HBM)
        analysis, inflation = pl.pallas_call(
            lambda *refs: kernel(regions, peers, *refs),
            out_shape=(
                pltpu.VMEM(ensemble.shape, BF16),
                jax.ShapeDtypeStruct((1, 1), F32),
            ),
            in_specs=[hbm] * 6,
            out_specs=(pl.BlockSpec(memory_space=pltpu.VMEM), pl.BlockSpec(memory_space=pltpu.SMEM)),
            scratch_shapes=scratch,
            compiler_params=pltpu.CompilerParams(
                collective_id=0, has_side_effects=True, vmem_limit_bytes=56 * 2**20
            ),
        )(
            ensemble,
            obs_weights,
            obs_tiles.reshape(1, n_obs),
            obs_values.reshape(1, n_obs),
            obs_error.reshape(1, n_obs),
            obs_noise,
        )
        return analysis, inflation.reshape(())

    return jax.shard_map(
        shards,
        mesh=mesh,
        in_specs=(
            P("depth", "member", "region"),
            P("depth"),
            P("region"),
            P("region"),
            P("region"),
            P("member", "region"),
        ),
        out_specs=(P("depth", "member", "region"), P()),
        check_vma=False,
    )
```

```python
import jax
import jax.numpy as jnp
from jax import lax
from jax.experimental import pallas as pl
from jax.experimental.pallas import tpu as pltpu
from jax.sharding import PartitionSpec as P

MEMBERS = 384
RADIUS = 1024.0
EARLY = 2
MESH = pl.DeviceIdType.MESH
F32 = jnp.float32
BF16 = jnp.bfloat16


def dot(a, b):
    return lax.dot_general(a, b, (((1,), (0,)), ((), ())), preferred_element_type=F32)


def kernel(
    regions,
    peers,
    ens_hbm,
    wts_hbm,
    tiles_hbm,
    vals_hbm,
    err_hbm,
    noise_hbm,
    out,
    infl_ref,
    ens,
    wts,
    spots,
    small,
    noise,
    blend,
    hot,
    part,
    obs,
    sums,
    slots,
    recv,
    back,
    anoms,
    means,
    anom_t,
    taper,
    gain,
    pert,
    tot,
    load_sem,
    e_send,
    e_recv,
    b_send,
    b_recv,
    o_send,
    o_recv,
    y_send,
    y_recv,
    n_send,
    n_recv,
    s_send,
    s_recv,
    d_send,
    d_recv,
    m_send,
    m_recv,
    i_send,
    i_recv,
    own_sem,
):
    n_var, own, n_tile = ens.shape
    n_obs = noise.shape[1]
    share = n_tile // peers
    r = lax.axis_index("region")
    d = lax.axis_index("depth")
    j = lax.axis_index("member")
    right, left, opp = lax.rem(j + 1, peers), lax.rem(j + 3, peers), lax.rem(j + 2, peers)
    after, before = lax.rem(r + 1, regions), lax.rem(r + regions - 1, regions)
    others = (right, left, opp)
    sides = (
        (0, after, r < regions - 1, r == regions // 2 - 1),
        (1, before, r > 0, r == regions // 2),
    )
    near = 2 * lax.rem(r + 1, 2)

    def rows(b):
        return pl.ds(pl.multiple_of(b * own, 16), own)

    def cols(b):
        return pl.ds(pl.multiple_of(b * share, 128), share)

    def half(h):
        return pl.ds(pl.multiple_of(h * (n_obs // 2), 128), n_obs // 2)

    def remote(src, dst, send, rec, **where):
        return pltpu.make_async_remote_copy(src, dst, send, rec, device_id=where, device_id_type=MESH)

    barrier = pltpu.get_barrier_semaphore()

    def greet(**where):
        pl.semaphore_signal(barrier, inc=1, device_id=where, device_id_type=MESH)

    def greet_region(o, c):
        greet(region=lax.rem(r + o, regions))
        return c

    lax.fori_loop(1, regions, greet_region, 0)
    for p in others:
        greet(member=p)
    greet(depth=1 - d)
    for k, p, has, seam in sides:

        @pl.when(seam)
        def _():
            greet(region=p, depth=1 - d)

    at_seam = jnp.logical_or(sides[0][3], sides[1][3]).astype(jnp.int32)

    loads = [
        pltpu.make_async_copy(ens_hbm, ens, load_sem.at[0]),
        pltpu.make_async_copy(wts_hbm, wts, load_sem.at[1]),
        pltpu.make_async_copy(tiles_hbm, spots, load_sem.at[2]),
        pltpu.make_async_copy(err_hbm, small.at[1, pl.ds(2, 1)], load_sem.at[3]),
        pltpu.make_async_copy(vals_hbm, small.at[1, pl.ds(1, 1)], load_sem.at[4]),
        pltpu.make_async_copy(noise_hbm, noise, load_sem.at[5]),
    ]
    for copy in loads:
        copy.start()

    def take_own(l):
        return pltpu.make_async_copy(ens_hbm.at[l, :, cols(j)], recv.at[l, rows(j), :], own_sem.at[l])

    lax.fori_loop(0, n_var, lambda l, c: (take_own(l).start(), c)[1], 0)

    def blended(i, c):
        at = pl.ds(pl.multiple_of(i * 16, 16), 16)
        total = wts[0] * ens[0, at, :].astype(F32)
        for l in range(1, n_var):
            total = total + wts[l] * ens[l, at, :].astype(F32)
        blend[at, :] = total.astype(BF16)
        return c

    with jax.named_scope("load_small"):
        loads[1].wait()
        loads[2].wait()
    tile_row = spots[...].astype(F32)
    small[1, 0:1, :] = tile_row

    def one_hot(i, c):
        at = pl.ds(pl.multiple_of(i * 128, 128), 128)
        index = (lax.broadcasted_iota(jnp.int32, (128, n_obs), 0) + i * 128).astype(F32)
        hot[at, :] = jnp.where(index == tile_row, 1.0, 0.0).astype(BF16)
        return c

    with jax.named_scope("hot"):
        lax.fori_loop(0, n_tile // 128, one_hot, 0)
    with jax.named_scope("noise"):
        for copy in loads[3:]:
            copy.wait()
        obs[1, 0, rows(j), :] = (jnp.sqrt(small[1, 2:3, :]) * noise[...]).astype(BF16)
    with jax.named_scope("blend"):
        loads[0].wait()
        lax.fori_loop(0, own // 16, blended, 0)
    with jax.named_scope("pick"):
        part[0] = dot(blend[...], hot[...]).astype(BF16)
    with jax.named_scope("barrier"):
        pl.semaphore_wait(barrier, regions + 3 + at_seam)

    def e_copies(l):
        return [
            remote(ens.at[l, :, cols(p)], recv.at[l, rows(j), :], e_send.at[k], e_recv.at[k, l], member=p)
            for k, p in enumerate(others)
        ]

    def send_ens(first, last):
        def body(l, c):
            for copy in e_copies(l):
                copy.start()
            return c

        lax.fori_loop(first, last, body, 0)

    def o_copies(q):
        block = obs.at[1, q, rows(j), half(d)]
        return [
            remote(block, block, o_send.at[q, k], o_recv.at[q, k], member=p) for k, p in enumerate(others)
        ]

    def to_depth(q, b):
        block = obs.at[1, q, rows(b), half(d)]
        remote(block, block, y_send.at[q], y_recv.at[q], depth=1 - d).start()

    def from_depth(q):
        three = obs.at[1, q, pl.ds(0, 3 * own), half(d)]
        return remote(three, three, y_send.at[q], y_recv.at[q], depth=1 - d)

    def to_beside(q, b, h=None):
        for k, p, has, seam in sides:

            def send(part, **where):
                at = (rows(b), slice(None)) if part is None else (rows(b), half(part))
                remote(
                    obs.at[(1, q) + at], obs.at[(2 * k, q) + at], n_send.at[q, k], n_recv.at[q, k], region=p, **where
                ).start()

            @pl.when(jnp.logical_and(has, jnp.logical_not(seam)))
            def _():
                send(h)

            if h is None or h is d:

                @pl.when(seam)
                def _():
                    send(d)
                    send(d, depth=1 - d)

    def beside(q, w):
        k = w // 2
        return remote(obs.at[1, q], obs.at[w, q], n_send.at[q, k], n_recv.at[q, k], region=after)

    def has_window(w):
        return jnp.logical_and(r + w > 0, r + w < regions + 1)

    def small_copy(k, p):
        return remote(small.at[1], small.at[2 * k], s_send.at[k], s_recv.at[k], region=p)

    swap = remote(part.at[0], part.at[1], d_send, d_recv, depth=1 - d)

    swap.start()
    for k, p, has, seam in sides:

        @pl.when(has)
        def _():
            small_copy(k, p).start()

    for copy in o_copies(0):
        copy.start()
    send_ens(0, EARLY)
    to_beside(0, j)

    with jax.named_scope("small"):
        for k, has in ((0, r > 0), (1, r < regions - 1)):

            @pl.when(has)
            def _():
                small_copy(k, after).wait_recv()

            @pl.when(jnp.logical_not(has))
            def _():
                small[2 * k] = jnp.ones_like(small[1])
                at = pl.ds(2 * k * n_obs, n_obs)
                anom_t[at, :] = jnp.zeros((n_obs, MEMBERS), BF16)
                gain[0, at, :] = jnp.zeros((n_obs, share), BF16)
                pert[:, at] = jnp.zeros((MEMBERS, n_obs), BF16)

    lane = lax.broadcasted_iota(jnp.int32, (n_obs, 128), 1) + j * share
    shifts = (
        jnp.where(r == 0, -16.0 * RADIUS, -RADIUS),
        jnp.float32(0.0),
        jnp.where(r == regions - 1, 16.0 * RADIUS, RADIUS),
    )
    with jax.named_scope("taper"):
        for w in range(3):
            spot = jnp.broadcast_to(small[w, 0:1, :] + shifts[w], (128, n_obs)).T
            for c in range(share // 128):
                level = jnp.maximum(0.0, 1.0 - jnp.abs((lane + c * 128).astype(F32) - spot) / RADIUS)
                taper[pl.ds(w * n_obs, n_obs), pl.ds(c * 128, 128)] = level * level / (MEMBERS - 1)

    with jax.named_scope("swap"):
        swap.wait_recv()
    mixed = (part[0].astype(F32) + part[1].astype(F32)).astype(BF16)
    obs[1, 1, rows(j), :] = mixed
    mixed = mixed.astype(F32)
    part_sum = jnp.sum(mixed, axis=0, keepdims=True)
    apart = mixed - part_sum / own
    sums[j, 0:1, :] = part_sum
    sums[j, 1:2, :] = jnp.sum(apart * apart, axis=0, keepdims=True)
    m_copies = [
        remote(sums.at[j], sums.at[j], m_send.at[k], m_recv.at[k], member=p) for k, p in enumerate(others)
    ]
    for copy in m_copies + o_copies(1):
        copy.start()
    to_beside(1, j)
    send_ens(EARLY, n_var)
    with jax.named_scope("noise_x"):
        for copy, b in zip(o_copies(0), (left, right, opp)):
            copy.wait_recv()
            to_depth(0, b)
            to_beside(0, b, d)

    with jax.named_scope("sums"):
        for copy in m_copies:
            copy.wait_recv()
    mean = (sums[0, 0:1, :] + sums[1, 0:1, :] + sums[2, 0:1, :] + sums[3, 0:1, :]) / MEMBERS
    squares = jnp.zeros_like(mean)
    for p in range(peers):
        off = sums[p, 0:1, :] / own - mean
        squares = squares + (sums[p, 1:2, :] + own * off * off)
    spread = squares / (MEMBERS - 1)
    tot[1, 0:1, :] = mean
    tot[1, 1:2, :] = spread
    innovation = small[1, 1:2, :] - mean
    line = lax.broadcasted_iota(jnp.int32, (8, 128), 0)
    slots[r] = jnp.where(
        line < 4,
        jnp.sum(innovation * innovation, axis=1, keepdims=True),
        jnp.sum(spread + small[1, 2:3, :], axis=1, keepdims=True),
    )

    def tell(o, c):
        remote(slots.at[r], slots.at[r], i_send, i_recv, region=lax.rem(r + o, regions)).start()
        return c

    lax.fori_loop(1, regions, tell, 0)
    told = slots.at[pl.ds(0, regions - 1)]
    tells = remote(told, told, i_send, i_recv, region=after)

    with jax.named_scope("pred_x"):
        for copy, b in zip(o_copies(1), (left, right, opp)):
            copy.wait_recv()
            to_depth(1, b)
            to_beside(1, b, d)
    with jax.named_scope("noise_y"):
        from_depth(0).wait_recv()
    for b in others:
        to_beside(0, b, 1 - d)
    def window(w):
        return pl.ds(pl.multiple_of(w * n_obs, n_obs), n_obs)

    def turned(w, mean):
        dev = obs[w, 1].astype(F32) - mean
        anom_t[window(w), :] = dev.T.astype(BF16)
        return dev

    def stats(w):
        mean = jnp.sum(obs[w, 1].astype(F32), axis=0, keepdims=True) / MEMBERS
        dev = turned(w, mean)
        tot[w, 0:1, :] = mean
        tot[w, 1:2, :] = jnp.sum(dev * dev, axis=0, keepdims=True) / (MEMBERS - 1)

    def anomalies_of(l, slot):
        with jax.named_scope("take"):
            take_own(l).wait()
            for copy in e_copies(l):
                copy.wait_recv()
        state = recv[l].astype(F32)
        mean = jnp.sum(state, axis=0, keepdims=True) / MEMBERS
        means[slot, 0:1, :] = mean
        anoms[slot] = (state - mean).astype(BF16)

    def gain_of(slot, w):
        at = window(w)
        gain[slot, at, :] = (dot(anom_t[at, :], anoms[slot]) * taper[at, :]).astype(BF16)

    def perturbed(w, infl, root):
        mean, spread = tot[w, 0:1, :], tot[w, 1:2, :]
        factor = infl / (infl * spread + small[w, 2:3, :])
        innovation = small[w, 1:2, :] - mean
        dev = obs[w, 1].astype(F32) - mean
        moved = innovation + obs[w, 0].astype(F32) - root * dev
        pert[:, window(w)] = (moved * factor).astype(BF16)

    with jax.named_scope("anom0"):
        anomalies_of(0, 0)
    with jax.named_scope("pred_y"):
        from_depth(1).wait_recv()
    for b in others:
        to_beside(1, b, 1 - d)
    with jax.named_scope("gain0"):
        turned(1, tot[1, 0:1, :])
        gain_of(0, 1)
    with jax.named_scope("infl"):
        tells.wait_recv()
    total = jnp.sum(slots[...], axis=0)
    infl = total[0:1, 0:1] / total[4:5, 0:1]
    root = jnp.sqrt(infl)
    infl_ref[...] = infl
    with jax.named_scope("pert1"):
        perturbed(1, infl, root)
    with jax.named_scope("near1"):
        beside(1, near).wait_recv()
    with jax.named_scope("gainn"):
        stats(near)
        gain_of(0, near)
    with jax.named_scope("near0"):
        beside(0, near).wait_recv()
    with jax.named_scope("pertn"):
        perturbed(near, infl, root)

    @pl.when(has_window(2 - near))
    def _():
        with jax.named_scope("far1"):
            beside(1, 2 - near).wait_recv()
        with jax.named_scope("gainf"):
            stats(2 - near)
            gain_of(0, 2 - near)
        with jax.named_scope("far0"):
            beside(0, 2 - near).wait_recv()
        with jax.named_scope("pertf"):
            perturbed(2 - near, infl, root)

    def b_copies(l):
        return [
            remote(back.at[l, rows(p), :], out.at[l, :, cols(j)], b_send.at[k], b_recv.at[k, l], member=p)
            for k, p in enumerate(others)
        ]

    def analyse(l, c):
        slot = lax.rem(l, 2)
        with jax.named_scope("inc"):
            increment = dot(pert[...], gain[slot])
            back[l] = (means[slot, 0:1, :] + root * anoms[slot].astype(F32) + increment).astype(BF16)
        for copy in b_copies(l):
            copy.start()
        out[l, :, cols(j)] = back[l, rows(j), :]

        @pl.when(l < n_var - 1)
        def _():
            with jax.named_scope("gain"):
                anomalies_of(l + 1, 1 - slot)
                for w in range(3):
                    gain_of(1 - slot, w)

        return c

    lax.fori_loop(0, n_var, analyse, 0)

    def finish(l, c):
        with jax.named_scope("fin"):
            for copy in b_copies(l):
                copy.wait_recv()
        return c

    lax.fori_loop(0, n_var, finish, 0)

    with jax.named_scope("sent"):
        whole = recv.at[:, pl.ds(0, own), :]
        for sems in (e_send, b_send):
            for k, p in enumerate(others):
                remote(whole, whole, sems.at[k], e_recv.at[0, 0], member=p).wait_send()
        for q in range(2):
            for copy in o_copies(q):
                copy.wait_send()
            from_depth(q).wait_send()
        for k, p, has, seam in sides:

            @pl.when(has)
            def _():
                small_copy(k, after).wait_send()
                for q in range(2):
                    beside(q, 2 * k).wait_send()

        for copy in m_copies:
            copy.wait_send()
        swap.wait_send()
        tells.wait_send()


def solution(mesh):
    regions, peers = mesh.shape["region"], mesh.shape["member"]

    def shards(ensemble, obs_weights, obs_tiles, obs_values, obs_error, obs_noise):
        n_var, own, n_tile = ensemble.shape
        n_obs = obs_tiles.shape[0]
        share, members = n_tile // peers, own * peers
        DMA = pltpu.SemaphoreType.DMA
        scratch = [
            pltpu.VMEM((n_var, own, n_tile), BF16),
            pltpu.SMEM((n_var,), F32),
            pltpu.VMEM((1, n_obs), jnp.int32),
            pltpu.VMEM((3, 8, n_obs), F32),
            pltpu.VMEM((own, n_obs), F32),
            pltpu.VMEM((own, n_tile), BF16),
            pltpu.VMEM((n_tile, n_obs), BF16),
            pltpu.VMEM((2, own, n_obs), BF16),
            pltpu.VMEM((3, 2, members, n_obs), BF16),
            pltpu.VMEM((peers, 8, n_obs), F32),
            pltpu.VMEM((regions, 8, 128), F32),
            pltpu.VMEM((n_var, members, share), BF16),
            pltpu.VMEM((n_var, members, share), BF16),
            pltpu.VMEM((2, members, share), BF16),
            pltpu.VMEM((2, 8, share), F32),
            pltpu.VMEM((3 * n_obs, members), BF16),
            pltpu.VMEM((3 * n_obs, share), F32),
            pltpu.VMEM((2, 3 * n_obs, share), BF16),
            pltpu.VMEM((members, 3 * n_obs), BF16),
            pltpu.VMEM((3, 8, n_obs), F32),
            DMA((6,)),
            DMA((3,)),
            DMA((3, n_var)),
            DMA((3,)),
            DMA((3, n_var)),
            DMA((2, 3)),
            DMA((2, 3)),
            DMA((2,)),
            DMA((2,)),
            DMA((2, 2)),
            DMA((2, 2)),
            DMA((2,)),
            DMA((2,)),
            DMA,
            DMA,
            DMA((3,)),
            DMA((3,)),
            DMA,
            DMA,
            DMA((n_var,)),
        ]
        hbm = pl.BlockSpec(memory_space=pltpu.HBM)
        analysis, inflation = pl.pallas_call(
            lambda *refs: kernel(regions, peers, *refs),
            out_shape=(
                pltpu.VMEM(ensemble.shape, BF16),
                pltpu.VMEM((1, 1), F32),
            ),
            in_specs=[hbm] * 6,
            out_specs=(pl.BlockSpec(memory_space=pltpu.VMEM), pl.BlockSpec(memory_space=pltpu.VMEM)),
            scratch_shapes=scratch,
            compiler_params=pltpu.CompilerParams(
                collective_id=0, has_side_effects=True, vmem_limit_bytes=56 * 2**20
            ),
        )(
            ensemble,
            obs_weights,
            obs_tiles.reshape(1, n_obs),
            obs_values.reshape(1, n_obs),
            obs_error.reshape(1, n_obs),
            obs_noise,
        )
        return analysis, inflation.reshape(())

    return jax.shard_map(
        shards,
        mesh=mesh,
        in_specs=(
            P("depth", "member", "region"),
            P("depth"),
            P("region"),
            P("region"),
            P("region"),
            P("member", "region"),
        ),
        out_specs=(P("depth", "member", "region"), P()),
        check_vma=False,
    )
```

```python
import jax
import jax.numpy as jnp
from jax import lax
from jax.experimental import pallas as pl
from jax.experimental.pallas import tpu as pltpu
from jax.sharding import PartitionSpec as P

MEMBERS = 384
RADIUS = 1024.0
RING = 4
EARLY = 1
MESH = pl.DeviceIdType.MESH
F32 = jnp.float32
BF16 = jnp.bfloat16


def dot(a, b):
    return lax.dot_general(a, b, (((1,), (0,)), ((), ())), preferred_element_type=F32)


def kernel(
    regions,
    peers,
    ring,
    ens_hbm,
    wts_hbm,
    tiles_hbm,
    vals_hbm,
    err_hbm,
    noise_hbm,
    out,
    infl_ref,
    ens,
    wts,
    spots,
    small,
    noise,
    blend,
    hot,
    part,
    obs,
    sums,
    slots,
    recv,
    back,
    anoms,
    means,
    anom_t,
    taper,
    gain,
    pert,
    tot,
    load_sem,
    e_send,
    e_recv,
    b_send,
    b_recv,
    o_send,
    o_recv,
    y_send,
    y_recv,
    n_send,
    n_recv,
    s_send,
    s_recv,
    d_send,
    d_recv,
    m_send,
    m_recv,
    i_send,
    i_recv,
    own_sem,
):
    n_var, own, n_tile = ens.shape
    n_obs = noise.shape[1]
    share = n_tile // peers
    r = lax.axis_index("region")
    d = lax.axis_index("depth")
    j = lax.axis_index("member")
    right, left, opp = lax.rem(j + 1, peers), lax.rem(j + 3, peers), lax.rem(j + 2, peers)
    after, before = lax.rem(r + 1, regions), lax.rem(r + regions - 1, regions)
    others = (right, left, opp)
    core, z, y = lax.rem(r, 2), lax.rem(r // 2, ring), r // (2 * ring)
    ring_peers = [r - 2 * z + 2 * lax.rem(z + o, ring) for o in range(1, ring)]
    across = r + 2 * ring * (1 - 2 * y)
    other_core = 1 - 2 * core
    sides = (
        (0, after, r < regions - 1, r == regions // 2 - 1),
        (1, before, r > 0, r == regions // 2),
    )
    near = 2 * lax.rem(r + 1, 2)

    def rows(b):
        return pl.ds(pl.multiple_of(b * own, 16), own)

    def cols(b):
        return pl.ds(pl.multiple_of(b * share, 128), share)

    def half(h):
        return pl.ds(pl.multiple_of(h * (n_obs // 2), 128), n_obs // 2)

    def remote(src, dst, send, rec, **where):
        return pltpu.make_async_remote_copy(src, dst, send, rec, device_id=where, device_id_type=MESH)

    barrier = pltpu.get_barrier_semaphore()

    def greet(**where):
        pl.semaphore_signal(barrier, inc=1, device_id=where, device_id_type=MESH)

    for p in others:
        greet(member=p)
    for p in ring_peers + [across, across + other_core]:
        greet(region=p)
    greet(depth=1 - d)
    for k, p, has, seam in sides:

        @pl.when(has)
        def _():
            greet(region=p)

        @pl.when(seam)
        def _():
            greet(region=p, depth=1 - d)

    greeted = ring + 5
    for k, p, has, seam in sides:
        greeted = greeted + has.astype(jnp.int32) + seam.astype(jnp.int32)

    loads = [
        pltpu.make_async_copy(ens_hbm, ens, load_sem.at[0]),
        pltpu.make_async_copy(wts_hbm, wts, load_sem.at[1]),
        pltpu.make_async_copy(tiles_hbm, spots, load_sem.at[2]),
        pltpu.make_async_copy(err_hbm, small.at[1, pl.ds(2, 1)], load_sem.at[3]),
        pltpu.make_async_copy(vals_hbm, small.at[1, pl.ds(1, 1)], load_sem.at[4]),
        pltpu.make_async_copy(noise_hbm, noise, load_sem.at[5]),
    ]
    for copy in loads:
        copy.start()

    def take_own(l):
        return pltpu.make_async_copy(ens_hbm.at[l, :, cols(j)], recv.at[l, rows(j), :], own_sem)

    lax.fori_loop(0, n_var, lambda l, c: (take_own(l).start(), c)[1], 0)

    def blended(i, c):
        at = pl.ds(pl.multiple_of(i * 16, 16), 16)
        total = wts[0] * ens[0, at, :].astype(F32)
        for l in range(1, n_var):
            total = total + wts[l] * ens[l, at, :].astype(F32)
        blend[at, :] = total.astype(BF16)
        return c

    with jax.named_scope("load_small"):
        loads[1].wait()
        loads[2].wait()
    tile_row = spots[...].astype(F32)
    small[1, 0:1, :] = tile_row

    def one_hot(i, c):
        at = pl.ds(pl.multiple_of(i * 128, 128), 128)
        index = (lax.broadcasted_iota(jnp.int32, (128, n_obs), 0) + i * 128).astype(F32)
        hot[at, :] = jnp.where(index == tile_row, 1.0, 0.0).astype(BF16)
        return c

    with jax.named_scope("hot"):
        lax.fori_loop(0, n_tile // 128, one_hot, 0)
    with jax.named_scope("noise"):
        for copy in loads[3:]:
            copy.wait()
        obs[1, 0, rows(j), :] = (jnp.sqrt(small[1, 2:3, :]) * noise[...]).astype(BF16)
    with jax.named_scope("ens"):
        loads[0].wait()
    with jax.named_scope("barrier"):
        pl.semaphore_wait(barrier, greeted)

    def e_copies(l):
        return [
            remote(ens.at[l, :, cols(p)], recv.at[l, rows(j), :], e_send, e_recv.at[l], member=p)
            for p in others
        ]

    def send_ens(first, last):
        def body(l, c):
            for copy in e_copies(l):
                copy.start()
            return c

        lax.fori_loop(first, last, body, 0)

    def o_copies(q):
        block = obs.at[1, q, rows(j), half(d)]
        return [
            remote(block, block, o_send, o_recv.at[q * (1 + k)], member=p) for k, p in enumerate(others)
        ]

    def over_depth(q, k, h):
        block = obs.at[1, q, rows((left, right, opp)[k]), half(h)]
        return remote(block, block, y_send, y_recv.at[q * (1 + k)], depth=1 - d)

    def to_depth(q, k):
        over_depth(q, k, d).start()

    def from_depth(q):
        if not q:
            three = obs.at[1, 0, pl.ds(0, 3 * own), half(1 - d)]
            remote(three, three, y_send, y_recv.at[0], depth=1 - d).wait_recv()
        for k, b in enumerate((left, right, opp)):
            if q:
                over_depth(q, k, 1 - d).wait_recv()
            to_beside(q, b, 1 - d)

    def to_beside(q, b, h=None):
        for k, p, has, seam in sides:

            def send(part, **where):
                at = (rows(b), slice(None)) if part is None else (rows(b), half(part))
                remote(
                    obs.at[(1, q) + at], obs.at[(2 * k, q) + at], n_send.at[k], n_recv.at[q, k], region=p, **where
                ).start()

            @pl.when(jnp.logical_and(has, jnp.logical_not(seam)))
            def _():
                send(h)

            if h is None or h is d:

                @pl.when(seam)
                def _():
                    send(d)
                    send(d, depth=1 - d)

    def take_half(q):
        if not q:
            three = obs.at[1, 0, pl.ds(0, 3 * own), half(d)]
            remote(three, three, o_send, o_recv.at[0], member=opp).wait_recv()
        for k, b in enumerate((left, right, opp)):
            if q:
                o_copies(q)[k].wait_recv()
            to_depth(q, k)
            to_beside(q, b, d)

    def beside(q, w):
        k = w // 2
        return remote(obs.at[1, q], obs.at[w, q], n_send.at[k], n_recv.at[q, k], region=after)

    def has_window(w):
        return jnp.logical_and(r + w > 0, r + w < regions + 1)

    def small_copy(k, p):
        return remote(small.at[1], small.at[2 * k], s_send.at[k], s_recv.at[k], region=p)

    swap = remote(part.at[0], part.at[1], d_send, d_recv, depth=1 - d)

    for copy in o_copies(0):
        copy.start()
    send_ens(0, EARLY)
    with jax.named_scope("blend"):
        lax.fori_loop(0, own // 16, blended, 0)
    with jax.named_scope("pick"):
        part[0] = dot(blend[...], hot[...]).astype(BF16)
    swap.start()
    for k, p, has, seam in sides:

        @pl.when(has)
        def _():
            small_copy(k, p).start()

    to_beside(0, j)

    with jax.named_scope("small"):
        for k, has in ((0, r > 0), (1, r < regions - 1)):

            @pl.when(has)
            def _():
                small_copy(k, after).wait_recv()

            @pl.when(jnp.logical_not(has))
            def _():
                small[2 * k] = jnp.ones_like(small[1])
                at = pl.ds(2 * k * n_obs, n_obs)
                anom_t[at, :] = jnp.zeros((n_obs, MEMBERS), BF16)
                gain[0, at, :] = jnp.zeros((n_obs, share), BF16)
                pert[:, at] = jnp.zeros((MEMBERS, n_obs), BF16)

    lane = lax.broadcasted_iota(jnp.int32, (n_obs, 128), 1) + j * share
    shifts = (
        jnp.where(r == 0, -16.0 * RADIUS, -RADIUS),
        jnp.float32(0.0),
        jnp.where(r == regions - 1, 16.0 * RADIUS, RADIUS),
    )
    with jax.named_scope("taper"):
        for w in range(3):
            spot = jnp.broadcast_to(small[w, 0:1, :] + shifts[w], (128, n_obs)).T
            for c in range(share // 128):
                level = jnp.maximum(0.0, 1.0 - jnp.abs((lane + c * 128).astype(F32) - spot) / RADIUS)
                taper[pl.ds(w * n_obs, n_obs), pl.ds(c * 128, 128)] = level * level / (MEMBERS - 1)

    with jax.named_scope("swap"):
        swap.wait_recv()
    mixed = (part[0].astype(F32) + part[1].astype(F32)).astype(BF16)
    obs[1, 1, rows(j), :] = mixed
    mixed = mixed.astype(F32)
    part_sum = jnp.sum(mixed, axis=0, keepdims=True)
    apart = mixed - part_sum / own
    sums[j, 0:1, :] = part_sum
    sums[j, 1:2, :] = jnp.sum(apart * apart, axis=0, keepdims=True)
    m_copies = [
        remote(sums.at[j], sums.at[j], m_send, m_recv, member=p) for p in others
    ]
    for copy in m_copies + o_copies(1):
        copy.start()
    to_beside(1, j)
    send_ens(EARLY, n_var)
    with jax.named_scope("noise_x"):
        take_half(0)

    with jax.named_scope("sums"):
        three_sums = sums.at[pl.ds(0, 3)]
        summed = remote(three_sums, three_sums, m_send, m_recv, member=opp)
        summed.wait_recv()
    mean = (sums[0, 0:1, :] + sums[1, 0:1, :] + sums[2, 0:1, :] + sums[3, 0:1, :]) / MEMBERS
    squares = jnp.zeros_like(mean)
    for p in range(peers):
        off = sums[p, 0:1, :] / own - mean
        squares = squares + (sums[p, 1:2, :] + own * off * off)
    spread = squares / (MEMBERS - 1)
    tot[1, 0:1, :] = mean
    tot[1, 1:2, :] = spread
    innovation = small[1, 1:2, :] - mean
    line = lax.broadcasted_iota(jnp.int32, (8, 128), 0)
    slots[0, z] = jnp.where(
        line < 4,
        jnp.sum(innovation * innovation, axis=1, keepdims=True),
        jnp.sum(spread + small[1, 2:3, :], axis=1, keepdims=True),
    )

    def tell(step, at, targets):
        for p in targets:
            remote(slots.at[step, at], slots.at[step, at], i_send.at[step], i_recv.at[step], region=p).start()

    def told(step):
        block = slots.at[step, pl.ds(0, 3)]
        return remote(block, block, i_send.at[step], i_recv.at[step], region=after)

    tell(0, z, ring_peers)
    with jax.named_scope("pred_x"):
        take_half(1)
    with jax.named_scope("noise_y"):
        from_depth(0)
    with jax.named_scope("told"):
        told(0).wait_recv()
        slots[1, 2 * y + core] = jnp.sum(slots[0], axis=0)
        tell(1, 2 * y + core, (r + other_core, across, across + other_core))
    def window(w):
        return pl.ds(pl.multiple_of(w * n_obs, n_obs), n_obs)

    def turned(w, mean):
        dev = obs[w, 1].astype(F32) - mean
        anom_t[window(w), :] = dev.T.astype(BF16)
        return dev

    def stats(w):
        mean = jnp.sum(obs[w, 1].astype(F32), axis=0, keepdims=True) / MEMBERS
        dev = turned(w, mean)
        tot[w, 0:1, :] = mean
        tot[w, 1:2, :] = jnp.sum(dev * dev, axis=0, keepdims=True) / (MEMBERS - 1)

    def anomalies_of(l, slot):
        with jax.named_scope("take"):
            block = recv.at[l, pl.ds(0, 3 * own), :]
            remote(block, block, e_send, e_recv.at[l], member=opp).wait_recv()
        state = recv[l].astype(F32)
        mean = jnp.sum(state, axis=0, keepdims=True) / MEMBERS
        means[slot, 0:1, :] = mean
        anoms[slot] = (state - mean).astype(BF16)

    def gain_of(slot, w):
        at = window(w)
        gain[slot, at, :] = (dot(anom_t[at, :], anoms[slot]) * taper[at, :]).astype(BF16)

    def perturbed(w, infl, root):
        mean, spread = tot[w, 0:1, :], tot[w, 1:2, :]
        factor = infl / (infl * spread + small[w, 2:3, :])
        innovation = small[w, 1:2, :] - mean
        dev = obs[w, 1].astype(F32) - mean
        moved = innovation + obs[w, 0].astype(F32) - root * dev
        pert[:, window(w)] = (moved * factor).astype(BF16)

    with jax.named_scope("anom0"):
        pltpu.make_async_copy(ens_hbm.at[:, :, cols(j)], recv.at[:, rows(j), :], own_sem).wait()
        anomalies_of(0, 0)
    with jax.named_scope("pred_y"):
        from_depth(1)
    with jax.named_scope("gain0"):
        turned(1, tot[1, 0:1, :])
        gain_of(0, 1)
    with jax.named_scope("infl"):
        told(1).wait_recv()
    total = jnp.sum(slots[1], axis=0)
    infl = total[0:1, 0:1] / total[4:5, 0:1]
    root = jnp.sqrt(infl)
    infl_ref[...] = infl
    with jax.named_scope("pert1"):
        perturbed(1, infl, root)
    with jax.named_scope("near1"):
        beside(1, near).wait_recv()
    with jax.named_scope("gainn"):
        stats(near)
        gain_of(0, near)
    with jax.named_scope("near0"):
        beside(0, near).wait_recv()
    with jax.named_scope("pertn"):
        perturbed(near, infl, root)

    @pl.when(has_window(2 - near))
    def _():
        with jax.named_scope("far1"):
            beside(1, 2 - near).wait_recv()
        with jax.named_scope("gainf"):
            stats(2 - near)
            gain_of(0, 2 - near)
        with jax.named_scope("far0"):
            beside(0, 2 - near).wait_recv()
        with jax.named_scope("pertf"):
            perturbed(2 - near, infl, root)

    def b_copies(l):
        return [
            remote(back.at[l, rows(p), :], out.at[l, :, cols(j)], b_send, b_recv, member=p)
            for k, p in enumerate(others)
        ]

    def analyse(l, c):
        slot = lax.rem(l, 2)
        with jax.named_scope("inc"):
            increment = dot(pert[...], gain[slot])
            back[l] = (means[slot, 0:1, :] + root * anoms[slot].astype(F32) + increment).astype(BF16)
        for copy in b_copies(l):
            copy.start()
        out[l, :, cols(j)] = back[l, rows(j), :]

        @pl.when(l < n_var - 1)
        def _():
            with jax.named_scope("gain"):
                anomalies_of(l + 1, 1 - slot)
                for w in range(3):
                    gain_of(1 - slot, w)

        return c

    lax.fori_loop(0, n_var, analyse, 0)

    with jax.named_scope("fin"):
        back_in = back.at[:, pl.ds(0, 3 * own), :]
        remote(back_in, back_in, b_send, b_recv, member=opp).wait_recv()

    with jax.named_scope("sent"):
        remote(back_in, back_in, b_send, b_recv, member=opp).wait_send()
        ens_in = recv.at[:, pl.ds(0, 3 * own), :]
        remote(ens_in, ens_in, e_send, e_recv.at[0], member=opp).wait_send()
        halves = obs.at[1, 0, pl.ds(0, 3 * own), :]
        remote(halves, halves, o_send, o_recv.at[0], member=opp).wait_send()
        remote(halves, halves, y_send, y_recv.at[0], depth=1 - d).wait_send()
        for k, p, has, seam in sides:

            @pl.when(has)
            def _():
                small_copy(k, after).wait_send()
                remote(obs.at[1], obs.at[2 * k], n_send.at[k], n_recv.at[0, k], region=after).wait_send()

        summed.wait_send()
        swap.wait_send()
        told(0).wait_send()
        told(1).wait_send()


def solution(mesh):
    regions, peers = mesh.shape["region"], mesh.shape["member"]

    def shards(ensemble, obs_weights, obs_tiles, obs_values, obs_error, obs_noise):
        n_var, own, n_tile = ensemble.shape
        n_obs = obs_tiles.shape[0]
        share, members = n_tile // peers, own * peers
        DMA = pltpu.SemaphoreType.DMA
        scratch = [
            pltpu.VMEM((n_var, own, n_tile), BF16),
            pltpu.SMEM((n_var,), F32),
            pltpu.VMEM((1, n_obs), jnp.int32),
            pltpu.VMEM((3, 8, n_obs), F32),
            pltpu.VMEM((own, n_obs), F32),
            pltpu.VMEM((own, n_tile), BF16),
            pltpu.VMEM((n_tile, n_obs), BF16),
            pltpu.VMEM((2, own, n_obs), BF16),
            pltpu.VMEM((3, 2, members, n_obs), BF16),
            pltpu.VMEM((peers, 2, n_obs), F32),
            pltpu.VMEM((2, RING, 8, 128), F32),
            pltpu.VMEM((n_var, members, share), BF16),
            pltpu.VMEM((n_var, members, share), BF16),
            pltpu.VMEM((2, members, share), BF16),
            pltpu.VMEM((2, 8, share), F32),
            pltpu.VMEM((3 * n_obs, members), BF16),
            pltpu.VMEM((3 * n_obs, share), F32),
            pltpu.VMEM((2, 3 * n_obs, share), BF16),
            pltpu.VMEM((members, 3 * n_obs), BF16),
            pltpu.VMEM((3, 8, n_obs), F32),
            DMA((6,)),
            DMA,
            DMA((n_var,)),
            DMA,
            DMA,
            DMA,
            DMA((4,)),
            DMA,
            DMA((4,)),
            DMA((2,)),
            DMA((2, 2)),
            DMA((2,)),
            DMA((2,)),
            DMA,
            DMA,
            DMA,
            DMA,
            DMA((2,)),
            DMA((2,)),
            DMA,
        ]
        hbm = pl.BlockSpec(memory_space=pltpu.HBM)
        analysis, inflation = pl.pallas_call(
            lambda *refs: kernel(regions, peers, RING, *refs),
            out_shape=(
                pltpu.VMEM(ensemble.shape, BF16),
                pltpu.VMEM((1, 1), F32),
            ),
            in_specs=[hbm] * 6,
            out_specs=(pl.BlockSpec(memory_space=pltpu.VMEM), pl.BlockSpec(memory_space=pltpu.VMEM)),
            scratch_shapes=scratch,
            compiler_params=pltpu.CompilerParams(
                collective_id=0, has_side_effects=True, vmem_limit_bytes=56 * 2**20
            ),
        )(
            ensemble,
            obs_weights,
            obs_tiles.reshape(1, n_obs),
            obs_values.reshape(1, n_obs),
            obs_error.reshape(1, n_obs),
            obs_noise,
        )
        return analysis, inflation.reshape(())

    return jax.shard_map(
        shards,
        mesh=mesh,
        in_specs=(
            P("depth", "member", "region"),
            P("depth"),
            P("region"),
            P("region"),
            P("region"),
            P("member", "region"),
        ),
        out_specs=(P("depth", "member", "region"), P()),
        check_vma=False,
    )
```

```python
import jax
import jax.numpy as jnp
from jax import lax
from jax.experimental import pallas as pl
from jax.experimental.pallas import tpu as pltpu
from jax.sharding import PartitionSpec as P

MEMBERS = 384
RADIUS = 1024.0
RING = 4
EARLY = 1
MESH = pl.DeviceIdType.MESH
F32 = jnp.float32
BF16 = jnp.bfloat16


def dot(a, b):
    return lax.dot_general(a, b, (((1,), (0,)), ((), ())), preferred_element_type=F32)


def kernel(
    regions,
    peers,
    ring,
    ens_hbm,
    wts_hbm,
    tiles_hbm,
    vals_hbm,
    err_hbm,
    noise_hbm,
    out,
    infl_ref,
    ens,
    wts,
    spots,
    small,
    noise,
    blend,
    hot,
    part,
    obs,
    sums,
    slots,
    recv,
    back,
    anoms,
    means,
    anom_t,
    taper,
    gain,
    pert,
    tot,
    load_sem,
    e_send,
    e_recv,
    b_send,
    b_recv,
    o_send,
    o_recv,
    y_send,
    y_recv,
    n_send,
    n_recv,
    s_send,
    s_recv,
    d_send,
    d_recv,
    m_send,
    m_recv,
    i_send,
    i_recv,
    own_sem,
):
    n_var, own, n_tile = ens.shape
    n_obs = noise.shape[1]
    share = n_tile // peers
    r = lax.axis_index("region")
    d = lax.axis_index("depth")
    j = lax.axis_index("member")
    right, left, opp = lax.rem(j + 1, peers), lax.rem(j + 3, peers), lax.rem(j + 2, peers)
    after, before = lax.rem(r + 1, regions), lax.rem(r + regions - 1, regions)
    others = (opp, right, left)
    core, z, y = lax.rem(r, 2), lax.rem(r // 2, ring), r // (2 * ring)
    ring_peers = [r - 2 * z + 2 * lax.rem(z + o, ring) for o in range(1, ring)]
    across = r + 2 * ring * (1 - 2 * y)
    other_core = 1 - 2 * core
    sides = (
        (0, after, r < regions - 1, r == regions // 2 - 1),
        (1, before, r > 0, r == regions // 2),
    )
    near = 2 * lax.rem(r + 1, 2)

    def rows(b):
        return pl.ds(pl.multiple_of(b * own, 16), own)

    def cols(b):
        return pl.ds(pl.multiple_of(b * share, 128), share)

    def half(h):
        return pl.ds(pl.multiple_of(h * (n_obs // 2), 128), n_obs // 2)

    def remote(src, dst, send, rec, **where):
        return pltpu.make_async_remote_copy(src, dst, send, rec, device_id=where, device_id_type=MESH)

    barrier = pltpu.get_barrier_semaphore()

    def greet(**where):
        pl.semaphore_signal(barrier, inc=1, device_id=where, device_id_type=MESH)

    for p in others:
        greet(member=p)
    for p in ring_peers + [across, across + other_core]:
        greet(region=p)
    greet(depth=1 - d)
    for k, p, has, seam in sides:

        @pl.when(has)
        def _():
            greet(region=p)

        @pl.when(seam)
        def _():
            greet(region=p, depth=1 - d)

    greeted = ring + 5
    for k, p, has, seam in sides:
        greeted = greeted + has.astype(jnp.int32) + seam.astype(jnp.int32)

    loads = [
        pltpu.make_async_copy(ens_hbm, ens, load_sem.at[0]),
        pltpu.make_async_copy(wts_hbm, wts, load_sem.at[1]),
        pltpu.make_async_copy(tiles_hbm, spots, load_sem.at[2]),
        pltpu.make_async_copy(err_hbm, small.at[1, pl.ds(2, 1)], load_sem.at[3]),
        pltpu.make_async_copy(vals_hbm, small.at[1, pl.ds(1, 1)], load_sem.at[4]),
        pltpu.make_async_copy(noise_hbm, noise, load_sem.at[5]),
    ]
    for copy in loads:
        copy.start()

    def take_own(l):
        return pltpu.make_async_copy(ens_hbm.at[l, :, cols(j)], recv.at[l, rows(j), :], own_sem)

    lax.fori_loop(0, n_var, lambda l, c: (take_own(l).start(), c)[1], 0)

    def blended(i, c):
        at = pl.ds(pl.multiple_of(i * 16, 16), 16)
        total = wts[0] * ens[0, at, :].astype(F32)
        for l in range(1, n_var):
            total = total + wts[l] * ens[l, at, :].astype(F32)
        blend[at, :] = total.astype(BF16)
        return c

    with jax.named_scope("load_small"):
        loads[1].wait()
        loads[2].wait()
    tile_row = spots[...].astype(F32)
    small[1, 0:1, :] = tile_row

    def one_hot(i, c):
        at = pl.ds(pl.multiple_of(i * 128, 128), 128)
        index = (lax.broadcasted_iota(jnp.int32, (128, n_obs), 0) + i * 128).astype(F32)
        hot[at, :] = jnp.where(index == tile_row, 1.0, 0.0).astype(BF16)
        return c

    with jax.named_scope("hot"):
        lax.fori_loop(0, n_tile // 128, one_hot, 0)
    with jax.named_scope("noise"):
        for copy in loads[3:]:
            copy.wait()
        obs[1, 0, rows(j), :] = (jnp.sqrt(small[1, 2:3, :]) * noise[...]).astype(BF16)
    with jax.named_scope("ens"):
        loads[0].wait()
    with jax.named_scope("barrier"):
        pl.semaphore_wait(barrier, greeted)

    def e_copies(l):
        return [
            remote(ens.at[l, :, cols(p)], recv.at[l, rows(j), :], e_send, e_recv.at[l], member=p)
            for p in others
        ]

    def send_ens(first, last):
        def body(l, c):
            for copy in e_copies(l):
                copy.start()
            return c

        lax.fori_loop(first, last, body, 0)

    def o_copies(q):
        block = obs.at[1, q, rows(j), half(d)]
        return [
            remote(block, block, o_send, o_recv.at[q * (1 + k)], member=p) for k, p in enumerate(others)
        ]

    def over_depth(q, k, h):
        block = obs.at[1, q, rows((opp, left, right)[k]), half(h)]
        return remote(block, block, y_send, y_recv.at[q * (1 + k)], depth=1 - d)

    def to_depth(q, k):
        over_depth(q, k, d).start()

    def from_depth(q):
        if not q:
            three = obs.at[1, 0, pl.ds(0, 3 * own), half(1 - d)]
            remote(three, three, y_send, y_recv.at[0], depth=1 - d).wait_recv()
        for k, b in enumerate((opp, left, right)):
            if q:
                over_depth(q, k, 1 - d).wait_recv()
            to_beside(q, b, 1 - d)

    def to_beside(q, b, h=None):
        for k, p, has, seam in sides:

            def send(part, **where):
                at = (rows(b), slice(None)) if part is None else (rows(b), half(part))
                remote(
                    obs.at[(1, q) + at], obs.at[(2 * k, q) + at], n_send.at[k], n_recv.at[q, k], region=p, **where
                ).start()

            @pl.when(jnp.logical_and(has, jnp.logical_not(seam)))
            def _():
                send(h)

            if h is None or h is d:

                @pl.when(seam)
                def _():
                    send(d)
                    send(d, depth=1 - d)

    def take_half(q):
        if not q:
            three = obs.at[1, 0, pl.ds(0, 3 * own), half(d)]
            remote(three, three, o_send, o_recv.at[0], member=opp).wait_recv()
        for k, b in enumerate((opp, left, right)):
            if q:
                o_copies(q)[k].wait_recv()
            to_depth(q, k)
            to_beside(q, b, d)

    def beside(q, w):
        k = w // 2
        return remote(obs.at[1, q], obs.at[w, q], n_send.at[k], n_recv.at[q, k], region=after)

    def has_window(w):
        return jnp.logical_and(r + w > 0, r + w < regions + 1)

    def small_copy(k, p):
        return remote(small.at[1], small.at[2 * k], s_send.at[k], s_recv.at[k], region=p)

    swap = remote(part.at[0], part.at[1], d_send, d_recv, depth=1 - d)

    for copy in o_copies(0):
        copy.start()
    send_ens(0, 1)
    for copy in e_copies(1)[:EARLY]:
        copy.start()
    with jax.named_scope("blend"):
        lax.fori_loop(0, own // 16, blended, 0)
    with jax.named_scope("pick"):
        part[0] = dot(blend[...], hot[...]).astype(BF16)
    swap.start()
    for k, p, has, seam in sides:

        @pl.when(has)
        def _():
            small_copy(k, p).start()

    to_beside(0, j)

    with jax.named_scope("small"):
        for k, has in ((0, r > 0), (1, r < regions - 1)):

            @pl.when(has)
            def _():
                small_copy(k, after).wait_recv()

            @pl.when(jnp.logical_not(has))
            def _():
                small[2 * k] = jnp.ones_like(small[1])
                at = pl.ds(2 * k * n_obs, n_obs)
                anom_t[at, :] = jnp.zeros((n_obs, MEMBERS), BF16)
                gain[0, at, :] = jnp.zeros((n_obs, share), BF16)
                pert[:, at] = jnp.zeros((MEMBERS, n_obs), BF16)

    lane = lax.broadcasted_iota(jnp.int32, (n_obs, 128), 1) + j * share
    shifts = (
        jnp.where(r == 0, -16.0 * RADIUS, -RADIUS),
        jnp.float32(0.0),
        jnp.where(r == regions - 1, 16.0 * RADIUS, RADIUS),
    )
    with jax.named_scope("taper"):
        for w in range(3):
            spot = jnp.broadcast_to(small[w, 0:1, :] + shifts[w], (128, n_obs)).T
            for c in range(share // 128):
                level = jnp.maximum(0.0, 1.0 - jnp.abs((lane + c * 128).astype(F32) - spot) / RADIUS)
                taper[pl.ds(w * n_obs, n_obs), pl.ds(c * 128, 128)] = level * level / (MEMBERS - 1)

    with jax.named_scope("swap"):
        swap.wait_recv()
    mixed = (part[0].astype(F32) + part[1].astype(F32)).astype(BF16)
    obs[1, 1, rows(j), :] = mixed
    mixed = mixed.astype(F32)
    part_sum = jnp.sum(mixed, axis=0, keepdims=True)
    apart = mixed - part_sum / own
    sums[j, 0:1, :] = part_sum
    sums[j, 1:2, :] = jnp.sum(apart * apart, axis=0, keepdims=True)
    m_copies = [
        remote(sums.at[j], sums.at[j], m_send, m_recv, member=p) for p in others
    ]
    for copy in m_copies + o_copies(1):
        copy.start()
    to_beside(1, j)
    for copy in e_copies(1)[EARLY:]:
        copy.start()
    send_ens(2, n_var)
    with jax.named_scope("noise_x"):
        take_half(0)

    with jax.named_scope("sums"):
        three_sums = sums.at[pl.ds(0, 3)]
        summed = remote(three_sums, three_sums, m_send, m_recv, member=opp)
        summed.wait_recv()
    mean = (sums[0, 0:1, :] + sums[1, 0:1, :] + sums[2, 0:1, :] + sums[3, 0:1, :]) / MEMBERS
    squares = jnp.zeros_like(mean)
    for p in range(peers):
        off = sums[p, 0:1, :] / own - mean
        squares = squares + (sums[p, 1:2, :] + own * off * off)
    spread = squares / (MEMBERS - 1)
    tot[1, 0:1, :] = mean
    tot[1, 1:2, :] = spread
    innovation = small[1, 1:2, :] - mean
    line = lax.broadcasted_iota(jnp.int32, (8, 128), 0)
    slots[0, z] = jnp.where(
        line < 4,
        jnp.sum(innovation * innovation, axis=1, keepdims=True),
        jnp.sum(spread + small[1, 2:3, :], axis=1, keepdims=True),
    )

    def tell(step, at, targets):
        for p in targets:
            remote(slots.at[step, at], slots.at[step, at], i_send.at[step], i_recv.at[step], region=p).start()

    def told(step):
        block = slots.at[step, pl.ds(0, 3)]
        return remote(block, block, i_send.at[step], i_recv.at[step], region=after)

    tell(0, z, ring_peers)
    with jax.named_scope("pred_x"):
        take_half(1)

    def tell_on():
        with jax.named_scope("told"):
            told(0).wait_recv()
            slots[1, 2 * y + core] = jnp.sum(slots[0], axis=0)
            tell(1, 2 * y + core, (r + other_core, across, across + other_core))

    pl.when(z == ring - 1)(tell_on)
    with jax.named_scope("noise_y"):
        from_depth(0)
    pl.when(z < ring - 1)(tell_on)
    def window(w):
        return pl.ds(pl.multiple_of(w * n_obs, n_obs), n_obs)

    def turned(w, mean):
        dev = obs[w, 1].astype(F32) - mean
        anom_t[window(w), :] = dev.astype(BF16).T
        return dev

    def stats(w):
        mean = jnp.sum(obs[w, 1].astype(F32), axis=0, keepdims=True) / MEMBERS
        dev = turned(w, mean)
        tot[w, 0:1, :] = mean
        tot[w, 1:2, :] = jnp.sum(dev * dev, axis=0, keepdims=True) / (MEMBERS - 1)

    def anomalies_of(l, slot):
        with jax.named_scope("take"):
            block = recv.at[l, pl.ds(0, 3 * own), :]
            remote(block, block, e_send, e_recv.at[l], member=opp).wait_recv()
        state = recv[l].astype(F32)
        mean = jnp.sum(state, axis=0, keepdims=True) / MEMBERS
        means[slot, 0:1, :] = mean
        anoms[slot] = (state - mean).astype(BF16)

    def gain_of(slot, w):
        at = window(w)
        gain[slot, at, :] = (dot(anom_t[at, :], anoms[slot]) * taper[at, :]).astype(BF16)

    def perturbed(w, infl, root):
        mean, spread = tot[w, 0:1, :], tot[w, 1:2, :]
        factor = infl / (infl * spread + small[w, 2:3, :])
        innovation = small[w, 1:2, :] - mean
        dev = obs[w, 1].astype(F32) - mean
        moved = innovation + obs[w, 0].astype(F32) - root * dev
        pert[:, window(w)] = (moved * factor).astype(BF16)

    with jax.named_scope("anom0"):
        pltpu.make_async_copy(ens_hbm.at[:, :, cols(j)], recv.at[:, rows(j), :], own_sem).wait()
        anomalies_of(0, 0)
    with jax.named_scope("pred_y"):
        from_depth(1)
    with jax.named_scope("gain0"):
        turned(1, tot[1, 0:1, :])
        gain_of(0, 1)
    with jax.named_scope("near1"):
        beside(1, near).wait_recv()
    with jax.named_scope("gainn"):
        stats(near)
        gain_of(0, near)

    def far_gain():
        with jax.named_scope("far1"):
            beside(1, 2 - near).wait_recv()
        with jax.named_scope("gainf"):
            stats(2 - near)
            gain_of(0, 2 - near)

    has_far = has_window(2 - near)
    pl.when(jnp.logical_and(has_far, core == 0))(far_gain)
    with jax.named_scope("infl"):
        told(1).wait_recv()
    total = jnp.sum(slots[1], axis=0)
    infl = total[0:1, 0:1] / total[4:5, 0:1]
    root = jnp.sqrt(infl)
    infl_ref[...] = infl
    with jax.named_scope("pert1"):
        perturbed(1, infl, root)
    with jax.named_scope("near0"):
        beside(0, near).wait_recv()
    with jax.named_scope("pertn"):
        perturbed(near, infl, root)

    pl.when(jnp.logical_and(has_far, core == 1))(far_gain)

    @pl.when(has_far)
    def _():
        with jax.named_scope("far0"):
            beside(0, 2 - near).wait_recv()
        with jax.named_scope("pertf"):
            perturbed(2 - near, infl, root)

    def b_copies(l):
        return [
            remote(back.at[l, rows(p), :], out.at[l, :, cols(j)], b_send, b_recv, member=p)
            for k, p in enumerate(others)
        ]

    def analyse(l, c):
        slot = lax.rem(l, 2)
        with jax.named_scope("inc"):
            increment = dot(pert[...], gain[slot])
            back[l] = (means[slot, 0:1, :] + root * anoms[slot].astype(F32) + increment).astype(BF16)
        for copy in b_copies(l):
            copy.start()
        out[l, :, cols(j)] = back[l, rows(j), :]

        @pl.when(l < n_var - 1)
        def _():
            with jax.named_scope("gain"):
                anomalies_of(l + 1, 1 - slot)
                for w in range(3):
                    gain_of(1 - slot, w)

        return c

    lax.fori_loop(0, n_var, analyse, 0)

    with jax.named_scope("fin"):
        back_in = back.at[:, pl.ds(0, 3 * own), :]
        remote(back_in, back_in, b_send, b_recv, member=opp).wait_recv()

    with jax.named_scope("sent"):
        remote(back_in, back_in, b_send, b_recv, member=opp).wait_send()
        ens_in = recv.at[:, pl.ds(0, 3 * own), :]
        remote(ens_in, ens_in, e_send, e_recv.at[0], member=opp).wait_send()
        halves = obs.at[1, 0, pl.ds(0, 3 * own), :]
        remote(halves, halves, o_send, o_recv.at[0], member=opp).wait_send()
        remote(halves, halves, y_send, y_recv.at[0], depth=1 - d).wait_send()
        for k, p, has, seam in sides:

            @pl.when(has)
            def _():
                small_copy(k, after).wait_send()
                remote(obs.at[1], obs.at[2 * k], n_send.at[k], n_recv.at[0, k], region=after).wait_send()

        summed.wait_send()
        swap.wait_send()
        told(0).wait_send()
        told(1).wait_send()


def solution(mesh):
    regions, peers = mesh.shape["region"], mesh.shape["member"]

    def shards(ensemble, obs_weights, obs_tiles, obs_values, obs_error, obs_noise):
        n_var, own, n_tile = ensemble.shape
        n_obs = obs_tiles.shape[0]
        share, members = n_tile // peers, own * peers
        DMA = pltpu.SemaphoreType.DMA
        scratch = [
            pltpu.VMEM((n_var, own, n_tile), BF16),
            pltpu.SMEM((n_var,), F32),
            pltpu.VMEM((1, n_obs), jnp.int32),
            pltpu.VMEM((3, 8, n_obs), F32),
            pltpu.VMEM((own, n_obs), F32),
            pltpu.VMEM((own, n_tile), BF16),
            pltpu.VMEM((n_tile, n_obs), BF16),
            pltpu.VMEM((2, own, n_obs), BF16),
            pltpu.VMEM((3, 2, members, n_obs), BF16),
            pltpu.VMEM((peers, 2, n_obs), F32),
            pltpu.VMEM((2, RING, 8, 128), F32),
            pltpu.VMEM((n_var, members, share), BF16),
            pltpu.VMEM((n_var, members, share), BF16),
            pltpu.VMEM((2, members, share), BF16),
            pltpu.VMEM((2, 8, share), F32),
            pltpu.VMEM((3 * n_obs, members), BF16),
            pltpu.VMEM((3 * n_obs, share), F32),
            pltpu.VMEM((2, 3 * n_obs, share), BF16),
            pltpu.VMEM((members, 3 * n_obs), BF16),
            pltpu.VMEM((3, 8, n_obs), F32),
            DMA((6,)),
            DMA,
            DMA((n_var,)),
            DMA,
            DMA,
            DMA,
            DMA((4,)),
            DMA,
            DMA((4,)),
            DMA((2,)),
            DMA((2, 2)),
            DMA((2,)),
            DMA((2,)),
            DMA,
            DMA,
            DMA,
            DMA,
            DMA((2,)),
            DMA((2,)),
            DMA,
        ]
        hbm = pl.BlockSpec(memory_space=pltpu.HBM)
        analysis, inflation = pl.pallas_call(
            lambda *refs: kernel(regions, peers, RING, *refs),
            out_shape=(
                pltpu.VMEM(ensemble.shape, BF16),
                pltpu.VMEM((1, 1), F32),
            ),
            in_specs=[hbm] * 6,
            out_specs=(pl.BlockSpec(memory_space=pltpu.VMEM), pl.BlockSpec(memory_space=pltpu.VMEM)),
            scratch_shapes=scratch,
            compiler_params=pltpu.CompilerParams(
                collective_id=0, has_side_effects=True, vmem_limit_bytes=56 * 2**20
            ),
        )(
            ensemble,
            obs_weights,
            obs_tiles.reshape(1, n_obs),
            obs_values.reshape(1, n_obs),
            obs_error.reshape(1, n_obs),
            obs_noise,
        )
        return analysis, inflation.reshape(())

    return jax.shard_map(
        shards,
        mesh=mesh,
        in_specs=(
            P("depth", "member", "region"),
            P("depth"),
            P("region"),
            P("region"),
            P("region"),
            P("member", "region"),
        ),
        out_specs=(P("depth", "member", "region"), P()),
        check_vma=False,
    )
```

```python
import jax
import jax.numpy as jnp
from jax import lax
from jax.experimental import pallas as pl
from jax.experimental.pallas import tpu as pltpu
from jax.sharding import PartitionSpec as P

MEMBERS = 384
RADIUS = 1024.0
RING = 4
CHUNK = 256
EARLY = 1
MESH = pl.DeviceIdType.MESH
F32 = jnp.float32
BF16 = jnp.bfloat16


def dot(a, b):
    return lax.dot_general(a, b, (((1,), (0,)), ((), ())), preferred_element_type=F32)


def kernel(
    regions,
    peers,
    ring,
    ens_hbm,
    wts_hbm,
    tiles_hbm,
    vals_hbm,
    err_hbm,
    noise_hbm,
    out,
    infl_ref,
    ens,
    wts,
    spots,
    small,
    noise,
    part,
    obs,
    sums,
    slots,
    recv,
    back,
    anoms,
    means,
    anom_t,
    taper,
    gain,
    pert,
    tot,
    load_sem,
    e_send,
    e_recv,
    b_send,
    b_recv,
    o_send,
    o_recv,
    y_send,
    y_recv,
    n_send,
    n_recv,
    s_send,
    s_recv,
    d_send,
    d_recv,
    m_send,
    m_recv,
    i_send,
    i_recv,
):
    n_var, own, n_tile = ens.shape
    n_obs = noise.shape[1]
    share = n_tile // peers
    r = lax.axis_index("region")
    d = lax.axis_index("depth")
    j = lax.axis_index("member")
    right, left, opp = lax.rem(j + 1, peers), lax.rem(j + 3, peers), lax.rem(j + 2, peers)
    after, before = lax.rem(r + 1, regions), lax.rem(r + regions - 1, regions)
    others = (opp, right, left)
    core, z, y = lax.rem(r, 2), lax.rem(r // 2, ring), r // (2 * ring)
    ring_peers = [r - 2 * z + 2 * lax.rem(z + o, ring) for o in range(1, ring)]
    across = r + 2 * ring * (1 - 2 * y)
    other_core = 1 - 2 * core
    sides = (
        (0, after, r < regions - 1, r == regions // 2 - 1),
        (1, before, r > 0, r == regions // 2),
    )
    near = 2 * lax.rem(r + 1, 2)

    def rows(b):
        return pl.ds(pl.multiple_of(b * own, 16), own)

    def cols(b):
        return pl.ds(pl.multiple_of(b * share, 128), share)

    def half(h):
        return pl.ds(pl.multiple_of(h * (n_obs // 2), 128), n_obs // 2)

    def remote(src, dst, send, rec, **where):
        return pltpu.make_async_remote_copy(src, dst, send, rec, device_id=where, device_id_type=MESH)

    barrier = pltpu.get_barrier_semaphore()

    def greet(**where):
        pl.semaphore_signal(barrier, inc=1, device_id=where, device_id_type=MESH)

    for p in others:
        greet(member=p)
    for p in ring_peers + [across, across + other_core]:
        greet(region=p)
    greet(depth=1 - d)
    for k, p, has, seam in sides:

        @pl.when(has)
        def _():
            greet(region=p)

        @pl.when(seam)
        def _():
            greet(region=p, depth=1 - d)

    greeted = ring + 5
    for k, p, has, seam in sides:
        greeted = greeted + has.astype(jnp.int32) + seam.astype(jnp.int32)

    loads = [
        pltpu.make_async_copy(ens_hbm, ens, load_sem.at[0]),
        pltpu.make_async_copy(wts_hbm, wts, load_sem.at[1]),
        pltpu.make_async_copy(tiles_hbm, spots, load_sem.at[2]),
        pltpu.make_async_copy(err_hbm, small.at[1, pl.ds(2, 1)], load_sem.at[3]),
        pltpu.make_async_copy(vals_hbm, small.at[1, pl.ds(1, 1)], load_sem.at[4]),
        pltpu.make_async_copy(noise_hbm, noise, load_sem.at[5]),
    ]
    for copy in loads:
        copy.start()

    with jax.named_scope("noise"):
        for copy in loads[3:]:
            copy.wait()
        obs[1, 0, rows(j), :] = (jnp.sqrt(small[1, 2:3, :]) * noise[...]).astype(BF16)
    with jax.named_scope("ens"):
        loads[0].wait()
    with jax.named_scope("barrier"):
        pl.semaphore_wait(barrier, greeted)

    def e_copies(l):
        return [
            remote(ens.at[l, :, cols(p)], recv.at[l, rows(j), :], e_send, e_recv.at[l], member=p)
            for p in others
        ]

    def send_ens(first, last):
        def body(l, c):
            for copy in e_copies(l):
                copy.start()
            return c

        lax.fori_loop(first, last, body, 0)

    last = n_var - 1

    def last_copies():
        to_right, to_left = dict(member=right), dict(member=left)
        return [
            remote(ens.at[last, :, cols(right)], recv.at[last, rows(j), :], e_send, e_recv.at[last + 2], **to_right),
            remote(ens.at[last, :, cols(opp)], recv.at[last + 1, rows(j), :], e_send, e_recv.at[last + 3], **to_left),
            remote(ens.at[last, :, cols(j)], recv.at[last + 1, rows(j), :], e_send, e_recv.at[last + 1], **to_right),
            remote(ens.at[last, :, cols(left)], recv.at[last, rows(j), :], e_send, e_recv.at[last], **to_left),
        ]

    def pass_on():
        first, second, _, _ = last_copies()
        block = recv.at[last, rows(left), :]
        first.wait_recv()
        remote(block, recv.at[last + 1, rows(left), :], e_send, e_recv.at[last + 1], member=right).start()
        block = recv.at[last + 1, rows(right), :]
        second.wait_recv()
        remote(block, recv.at[last, rows(right), :], e_send, e_recv.at[last], member=left).start()

    def o_copies(q):
        block = obs.at[1, q, rows(j), half(d)]
        return [
            remote(block, block, o_send, o_recv.at[q * (1 + k)], member=p) for k, p in enumerate(others)
        ]

    def over_depth(q, k, h):
        block = obs.at[1, q, rows((opp, left, right)[k]), half(h)]
        return remote(block, block, y_send, y_recv.at[q * (1 + k)], depth=1 - d)

    def to_depth(q, k):
        over_depth(q, k, d).start()

    def from_depth(q):
        if not q:
            three = obs.at[1, 0, pl.ds(0, 3 * own), half(1 - d)]
            remote(three, three, y_send, y_recv.at[0], depth=1 - d).wait_recv()
        for k, b in enumerate((opp, left, right)):
            if q:
                over_depth(q, k, 1 - d).wait_recv()
            to_beside(q, b, 1 - d)

    def to_beside(q, b, h=None):
        for k, p, has, seam in sides:

            def send(part, **where):
                at = (rows(b), slice(None)) if part is None else (rows(b), half(part))
                remote(
                    obs.at[(1, q) + at], obs.at[(2 * k, q) + at], n_send.at[k], n_recv.at[q, k], region=p, **where
                ).start()

            @pl.when(jnp.logical_and(has, jnp.logical_not(seam)))
            def _():
                send(h)

            if h is None or h is d:

                @pl.when(seam)
                def _():
                    send(d)
                    send(d, depth=1 - d)

    def take_half(q):
        if not q:
            three = obs.at[1, 0, pl.ds(0, 3 * own), half(d)]
            remote(three, three, o_send, o_recv.at[0], member=opp).wait_recv()
        for k, b in enumerate((opp, left, right)):
            if q:
                o_copies(q)[k].wait_recv()
            to_depth(q, k)
            to_beside(q, b, d)

    def beside(q, w):
        k = w // 2
        return remote(obs.at[1, q], obs.at[w, q], n_send.at[k], n_recv.at[q, k], region=after)

    def has_window(w):
        return jnp.logical_and(r + w > 0, r + w < regions + 1)

    def small_copy(k, p):
        return remote(small.at[1], small.at[2 * k], s_send.at[k], s_recv.at[k], region=p)

    swap = remote(part.at[0], part.at[1], d_send, d_recv, depth=1 - d)

    for copy in o_copies(0):
        copy.start()
    send_ens(0, 1)
    for copy in e_copies(1)[:EARLY]:
        copy.start()

    with jax.named_scope("load_small"):
        loads[1].wait()
        loads[2].wait()
    with jax.named_scope("pick"):
        spot_row = spots[...]
        picked = None
        for c in range(n_tile // CHUNK):
            at = pl.ds(c * CHUNK, CHUNK)
            index = lax.broadcasted_iota(jnp.int32, (CHUNK, n_obs), 0) + c * CHUNK
            hot = jnp.where(index == spot_row, 1.0, 0.0).astype(BF16)
            blend = wts[0] * ens[0, :, at].astype(F32)
            for l in range(1, n_var):
                blend = blend + wts[l] * ens[l, :, at].astype(F32)
            term = dot(blend.astype(BF16), hot)
            picked = term if picked is None else picked + term
        part[0] = picked.astype(BF16)
    swap.start()
    small[1, 0:1, :] = spot_row.astype(F32)
    for k, p, has, seam in sides:

        @pl.when(has)
        def _():
            small_copy(k, p).start()

    to_beside(0, j)

    def take_own(l, c):
        recv[l, rows(j), :] = ens[l, :, cols(j)]
        return c

    lax.fori_loop(0, n_var, take_own, 0)
    recv[last + 1, rows(j), :] = ens[last, :, cols(left)]

    with jax.named_scope("swap"):
        swap.wait_recv()
    mixed = (part[0].astype(F32) + part[1].astype(F32)).astype(BF16)
    obs[1, 1, rows(j), :] = mixed
    mixed = mixed.astype(F32)
    part_sum = jnp.sum(mixed, axis=0, keepdims=True)
    apart = mixed - part_sum / own
    sums[j, 0:1, :] = part_sum
    sums[j, 1:2, :] = jnp.sum(apart * apart, axis=0, keepdims=True)
    m_copies = [
        remote(sums.at[j], sums.at[j], m_send, m_recv, member=p) for p in others
    ]
    for copy in m_copies + o_copies(1):
        copy.start()
    to_beside(1, j)
    for copy in last_copies():
        copy.start()
    for copy in e_copies(1)[EARLY:]:
        copy.start()
    send_ens(2, last)
    with jax.named_scope("noise_x"):
        take_half(0)

    with jax.named_scope("small"):
        for k, has in ((0, r > 0), (1, r < regions - 1)):

            @pl.when(has)
            def _():
                small_copy(k, after).wait_recv()

            @pl.when(jnp.logical_not(has))
            def _():
                small[2 * k] = jnp.ones_like(small[1])
                at = pl.ds(2 * k * n_obs, n_obs)
                anom_t[at, :] = jnp.zeros((n_obs, MEMBERS), BF16)
                gain[0, at, :] = jnp.zeros((n_obs, share), BF16)
                pert[:, at] = jnp.zeros((MEMBERS, n_obs), BF16)

    lane = lax.broadcasted_iota(jnp.int32, (n_obs, 128), 1)
    shifts = (
        jnp.where(r == 0, -16.0 * RADIUS, -RADIUS),
        jnp.float32(0.0),
        jnp.where(r == regions - 1, 16.0 * RADIUS, RADIUS),
    )
    with jax.named_scope("taper"):
        for w in range(3):
            spot = jnp.broadcast_to(small[w, 0:1, :] + shifts[w], (128, n_obs)).T
            for k, quarter in enumerate((j, left)):
                for c in range(share // 128):
                    tile = (lane + (quarter * share + c * 128)).astype(F32)
                    level = jnp.maximum(0.0, 1.0 - jnp.abs(tile - spot) / RADIUS)
                    taper[k, pl.ds(w * n_obs, n_obs), pl.ds(c * 128, 128)] = level * level / (MEMBERS - 1)

    with jax.named_scope("sums"):
        three_sums = sums.at[pl.ds(0, 3)]
        summed = remote(three_sums, three_sums, m_send, m_recv, member=opp)
        summed.wait_recv()
    mean = (sums[0, 0:1, :] + sums[1, 0:1, :] + sums[2, 0:1, :] + sums[3, 0:1, :]) / MEMBERS
    squares = jnp.zeros_like(mean)
    for p in range(peers):
        off = sums[p, 0:1, :] / own - mean
        squares = squares + (sums[p, 1:2, :] + own * off * off)
    spread = squares / (MEMBERS - 1)
    tot[1, 0:1, :] = mean
    tot[1, 1:2, :] = spread
    innovation = small[1, 1:2, :] - mean
    line = lax.broadcasted_iota(jnp.int32, (8, 128), 0)
    slots[0, z] = jnp.where(
        line < 4,
        jnp.sum(innovation * innovation, axis=1, keepdims=True),
        jnp.sum(spread + small[1, 2:3, :], axis=1, keepdims=True),
    )

    def tell(step, at, targets):
        for p in targets:
            remote(slots.at[step, at], slots.at[step, at], i_send.at[step], i_recv.at[step], region=p).start()

    def told(step):
        block = slots.at[step, pl.ds(0, 3)]
        return remote(block, block, i_send.at[step], i_recv.at[step], region=after)

    tell(0, z, ring_peers)
    with jax.named_scope("pred_x"):
        take_half(1)

    def tell_on():
        with jax.named_scope("told"):
            told(0).wait_recv()
            slots[1, 2 * y + core] = jnp.sum(slots[0], axis=0)
            tell(1, 2 * y + core, (r + other_core, across, across + other_core))

    pl.when(z == ring - 1)(tell_on)
    with jax.named_scope("noise_y"):
        from_depth(0)
    pl.when(z < ring - 1)(tell_on)
    def window(w):
        return pl.ds(pl.multiple_of(w * n_obs, n_obs), n_obs)

    def turned(w, mean):
        dev = obs[w, 1].astype(F32) - mean
        anom_t[window(w), :] = dev.astype(BF16).T
        return dev

    def stats(w):
        mean = jnp.sum(obs[w, 1].astype(F32), axis=0, keepdims=True) / MEMBERS
        dev = turned(w, mean)
        tot[w, 0:1, :] = mean
        tot[w, 1:2, :] = jnp.sum(dev * dev, axis=0, keepdims=True) / (MEMBERS - 1)

    def anomalies_of(l, slot):
        with jax.named_scope("take"):
            for count, here in ((3, l < last), (2, l >= last)):

                @pl.when(here)
                def _():
                    block = recv.at[l, pl.ds(0, count * own), :]
                    remote(block, block, e_send, e_recv.at[l], member=opp).wait_recv()

        state = recv[l].astype(F32)
        mean = jnp.sum(state, axis=0, keepdims=True) / MEMBERS
        means[slot, 0:1, :] = mean
        anoms[slot] = (state - mean).astype(BF16)

    def gain_of(slot, w, quarter=0):
        at = window(w)
        gain[slot, at, :] = (dot(anom_t[at, :], anoms[slot]) * taper[quarter, at, :]).astype(BF16)

    def perturbed(w, infl, root):
        mean, spread = tot[w, 0:1, :], tot[w, 1:2, :]
        factor = infl / (infl * spread + small[w, 2:3, :])
        innovation = small[w, 1:2, :] - mean
        dev = obs[w, 1].astype(F32) - mean
        moved = innovation + obs[w, 0].astype(F32) - root * dev
        pert[:, window(w)] = (moved * factor).astype(BF16)

    with jax.named_scope("anom0"):
        anomalies_of(0, 0)
    with jax.named_scope("pass"):
        pass_on()
    with jax.named_scope("pred_y"):
        from_depth(1)
    with jax.named_scope("gain0"):
        turned(1, tot[1, 0:1, :])
        gain_of(0, 1)
    with jax.named_scope("near1"):
        beside(1, near).wait_recv()
    with jax.named_scope("gainn"):
        stats(near)
        gain_of(0, near)

    def far_gain():
        with jax.named_scope("far1"):
            beside(1, 2 - near).wait_recv()
        with jax.named_scope("gainf"):
            stats(2 - near)
            gain_of(0, 2 - near)

    has_far = has_window(2 - near)
    pl.when(jnp.logical_and(has_far, core == 0))(far_gain)
    with jax.named_scope("infl"):
        told(1).wait_recv()
    total = jnp.sum(slots[1], axis=0)
    infl = total[0:1, 0:1] / total[4:5, 0:1]
    root = jnp.sqrt(infl)
    infl_ref[...] = infl
    with jax.named_scope("pert1"):
        perturbed(1, infl, root)
    with jax.named_scope("near0"):
        beside(0, near).wait_recv()
    with jax.named_scope("pertn"):
        perturbed(near, infl, root)

    pl.when(jnp.logical_and(has_far, core == 1))(far_gain)

    @pl.when(has_far)
    def _():
        with jax.named_scope("far0"):
            beside(0, 2 - near).wait_recv()
        with jax.named_scope("pertf"):
            perturbed(2 - near, infl, root)

    def b_copies(l):
        return [
            remote(back.at[l, rows(p), :], out.at[l, :, cols(j)], b_send, b_recv, member=p)
            for k, p in enumerate(others)
        ]

    def analyse(l, c):
        slot = lax.rem(l, 2)
        with jax.named_scope("inc"):
            increment = dot(pert[...], gain[slot])
            back[l] = (means[slot, 0:1, :] + root * anoms[slot].astype(F32) + increment).astype(BF16)

        @pl.when(l < last)
        def _():
            for copy in b_copies(l):
                copy.start()
            out[l, :, cols(j)] = back[l, rows(j), :]

        for k, quarter, p in ((last, j, left), (last + 1, left, right)):

            @pl.when(l == k)
            def _():
                remote(
                    back.at[k, rows(p), :], out.at[last, :, cols(quarter)], b_send, b_recv, member=p
                ).start()
                out[last, :, cols(quarter)] = back[k, rows(j), :]

        @pl.when(l <= last)
        def _():
            with jax.named_scope("gain"):
                anomalies_of(l + 1, 1 - slot)
                for w in range(3):
                    gain_of(1 - slot, w, (l + 1) // n_var)

        return c

    lax.fori_loop(0, n_var + 1, analyse, 0)

    with jax.named_scope("fin"):
        back_in = back.at[pl.ds(0, 5)]
        remote(back_in, back_in, b_send, b_recv, member=opp).wait_recv()

    with jax.named_scope("sent"):
        remote(back_in, back_in, b_send, b_recv, member=opp).wait_send()
        ens_in = recv.at[pl.ds(0, 6)]
        remote(ens_in, ens_in, e_send, e_recv.at[0], member=opp).wait_send()
        halves = obs.at[1, 0, pl.ds(0, 3 * own), :]
        remote(halves, halves, o_send, o_recv.at[0], member=opp).wait_send()
        remote(halves, halves, y_send, y_recv.at[0], depth=1 - d).wait_send()
        for k, p, has, seam in sides:

            @pl.when(has)
            def _():
                small_copy(k, after).wait_send()
                remote(obs.at[1], obs.at[2 * k], n_send.at[k], n_recv.at[0, k], region=after).wait_send()

        summed.wait_send()
        swap.wait_send()
        told(0).wait_send()
        told(1).wait_send()


def solution(mesh):
    regions, peers = mesh.shape["region"], mesh.shape["member"]

    def shards(ensemble, obs_weights, obs_tiles, obs_values, obs_error, obs_noise):
        n_var, own, n_tile = ensemble.shape
        n_obs = obs_tiles.shape[0]
        share, members = n_tile // peers, own * peers
        DMA = pltpu.SemaphoreType.DMA
        scratch = [
            pltpu.VMEM((n_var, own, n_tile), BF16),
            pltpu.SMEM((n_var,), F32),
            pltpu.VMEM((1, n_obs), jnp.int32),
            pltpu.VMEM((3, 8, n_obs), F32),
            pltpu.VMEM((own, n_obs), F32),
            pltpu.VMEM((2, own, n_obs), BF16),
            pltpu.VMEM((3, 2, members, n_obs), BF16),
            pltpu.VMEM((peers, 2, n_obs), F32),
            pltpu.VMEM((2, RING, 8, 128), F32),
            pltpu.VMEM((n_var + 1, members, share), BF16),
            pltpu.VMEM((n_var + 1, members, share), BF16),
            pltpu.VMEM((2, members, share), BF16),
            pltpu.VMEM((2, 8, share), F32),
            pltpu.VMEM((3 * n_obs, members), BF16),
            pltpu.VMEM((2, 3 * n_obs, share), F32),
            pltpu.VMEM((2, 3 * n_obs, share), BF16),
            pltpu.VMEM((members, 3 * n_obs), BF16),
            pltpu.VMEM((3, 8, n_obs), F32),
            DMA((6,)),
            DMA,
            DMA((n_var + 3,)),
            DMA,
            DMA,
            DMA,
            DMA((4,)),
            DMA,
            DMA((4,)),
            DMA((2,)),
            DMA((2, 2)),
            DMA((2,)),
            DMA((2,)),
            DMA,
            DMA,
            DMA,
            DMA,
            DMA((2,)),
            DMA((2,)),
        ]
        hbm = pl.BlockSpec(memory_space=pltpu.HBM)
        analysis, inflation = pl.pallas_call(
            lambda *refs: kernel(regions, peers, RING, *refs),
            out_shape=(
                pltpu.VMEM(ensemble.shape, BF16),
                pltpu.VMEM((1, 1), F32),
            ),
            in_specs=[hbm] * 6,
            out_specs=(pl.BlockSpec(memory_space=pltpu.VMEM), pl.BlockSpec(memory_space=pltpu.VMEM)),
            scratch_shapes=scratch,
            compiler_params=pltpu.CompilerParams(
                collective_id=0, has_side_effects=True, vmem_limit_bytes=56 * 2**20
            ),
        )(
            ensemble,
            obs_weights,
            obs_tiles.reshape(1, n_obs),
            obs_values.reshape(1, n_obs),
            obs_error.reshape(1, n_obs),
            obs_noise,
        )
        return analysis, inflation.reshape(())

    return jax.shard_map(
        shards,
        mesh=mesh,
        in_specs=(
            P("depth", "member", "region"),
            P("depth"),
            P("region"),
            P("region"),
            P("region"),
            P("member", "region"),
        ),
        out_specs=(P("depth", "member", "region"), P()),
        check_vma=False,
    )
```

```python
import jax
import jax.numpy as jnp
from jax import lax
from jax.experimental import pallas as pl
from jax.experimental.pallas import tpu as pltpu
from jax.sharding import PartitionSpec as P

MEMBERS = 384
RADIUS = 1024.0
RING = 4
CHUNK = 256
TWICE = 2
EARLY = 3
MESH = pl.DeviceIdType.MESH
F32 = jnp.float32
BF16 = jnp.bfloat16


def dot(a, b):
    return lax.dot_general(a, b, (((1,), (0,)), ((), ())), preferred_element_type=F32)


def kernel(
    regions,
    peers,
    ring,
    ens_hbm,
    wts_hbm,
    tiles_hbm,
    vals_hbm,
    err_hbm,
    noise_hbm,
    out,
    infl_ref,
    ens,
    wts,
    spots,
    small,
    noise,
    part,
    obs,
    sums,
    slots,
    recv,
    back,
    anoms,
    means,
    anom_t,
    taper,
    gain,
    pert,
    tot,
    load_sem,
    e_send,
    e_recv,
    b_send,
    b_recv,
    o_send,
    o_recv,
    y_send,
    y_recv,
    n_send,
    n_recv,
    s_send,
    s_recv,
    d_send,
    d_recv,
    m_send,
    m_recv,
    i_send,
    i_recv,
):
    n_var, own, n_tile = ens.shape
    n_obs = noise.shape[1]
    share = n_tile // peers
    r = lax.axis_index("region")
    d = lax.axis_index("depth")
    j = lax.axis_index("member")
    right, left, opp = lax.rem(j + 1, peers), lax.rem(j + 3, peers), lax.rem(j + 2, peers)
    after, before = lax.rem(r + 1, regions), lax.rem(r + regions - 1, regions)
    others = (opp, right, left)
    core, z, y = lax.rem(r, 2), lax.rem(r // 2, ring), r // (2 * ring)
    ring_peers = [r - 2 * z + 2 * lax.rem(z + o, ring) for o in range(1, ring)]
    across = r + 2 * ring * (1 - 2 * y)
    other_core = 1 - 2 * core
    sides = (
        (0, after, r < regions - 1, r == regions // 2 - 1),
        (1, before, r > 0, r == regions // 2),
    )
    near = 2 * lax.rem(r + 1, 2)

    def rows(b):
        return pl.ds(pl.multiple_of(b * own, 16), own)

    def cols(b):
        return pl.ds(pl.multiple_of(b * share, 128), share)

    def half(h):
        return pl.ds(pl.multiple_of(h * (n_obs // 2), 128), n_obs // 2)

    def remote(src, dst, send, rec, **where):
        return pltpu.make_async_remote_copy(src, dst, send, rec, device_id=where, device_id_type=MESH)

    barrier = pltpu.get_barrier_semaphore()

    def greet(**where):
        pl.semaphore_signal(barrier, inc=1, device_id=where, device_id_type=MESH)

    for p in others:
        greet(member=p)
    for p in ring_peers + [across, across + other_core]:
        greet(region=p)
    greet(depth=1 - d)
    for k, p, has, seam in sides:

        @pl.when(has)
        def _():
            greet(region=p)

        @pl.when(seam)
        def _():
            greet(region=p, depth=1 - d)

    greeted = ring + 5
    for k, p, has, seam in sides:
        greeted = greeted + has.astype(jnp.int32) + seam.astype(jnp.int32)

    rest = pl.ds(1, n_var - 1)
    loads = [
        pltpu.make_async_copy(err_hbm, small.at[1, pl.ds(2, 1)], load_sem.at[0]),
        pltpu.make_async_copy(noise_hbm, noise, load_sem.at[1]),
        pltpu.make_async_copy(ens_hbm.at[0], ens.at[0], load_sem.at[2]),
        pltpu.make_async_copy(tiles_hbm, spots, load_sem.at[3]),
        pltpu.make_async_copy(wts_hbm, wts, load_sem.at[4]),
        pltpu.make_async_copy(ens_hbm.at[rest], ens.at[rest], load_sem.at[5]),
        pltpu.make_async_copy(vals_hbm, small.at[1, pl.ds(1, 1)], load_sem.at[6]),
    ]
    for copy in loads:
        copy.start()

    with jax.named_scope("noise"):
        loads[0].wait()
        loads[1].wait()
        obs[1, 0, rows(j), :] = (jnp.sqrt(small[1, 2:3, :]) * noise[...]).astype(BF16)
    with jax.named_scope("ens"):
        loads[2].wait()
    with jax.named_scope("barrier"):
        pl.semaphore_wait(barrier, greeted)

    def e_copies(l):
        return [
            remote(ens.at[l, :, cols(p)], recv.at[l, rows(j), :], e_send, e_recv.at[l], member=p)
            for p in others
        ]

    def send_ens(first, last):
        def body(l, c):
            for copy in e_copies(l):
                copy.start()
            return c

        lax.fori_loop(first, last, body, 0)

    first = n_var - TWICE

    def twice_copies(l):
        far, rec = l + TWICE, n_var + TWICE + 2 * (l - first)
        return [
            remote(ens.at[l, :, cols(right)], recv.at[l, rows(j), :], e_send, e_recv.at[rec], member=right),
            remote(ens.at[l, :, cols(opp)], recv.at[far, rows(j), :], e_send, e_recv.at[rec + 1], member=left),
            remote(ens.at[l, :, cols(j)], recv.at[far, rows(j), :], e_send, e_recv.at[far], member=right),
            remote(ens.at[l, :, cols(left)], recv.at[l, rows(j), :], e_send, e_recv.at[l], member=left),
        ]

    def pass_on(l):
        far, copies = l + TWICE, twice_copies(l)
        block = recv.at[l, rows(left), :]
        copies[0].wait_recv()
        remote(block, recv.at[far, rows(left), :], e_send, e_recv.at[far], member=right).start()
        block = recv.at[far, rows(right), :]
        copies[1].wait_recv()
        remote(block, recv.at[l, rows(right), :], e_send, e_recv.at[l], member=left).start()

    def o_copies(q):
        block = obs.at[1, q, rows(j), half(d)]
        return [
            remote(block, block, o_send, o_recv.at[q * (1 + k)], member=p) for k, p in enumerate(others)
        ]

    def over_depth(q, k, h):
        block = obs.at[1, q, rows((opp, left, right)[k]), half(h)]
        return remote(block, block, y_send, y_recv.at[q * (1 + k)], depth=1 - d)

    def to_depth(q, k):
        over_depth(q, k, d).start()

    def from_depth(q):
        if not q:
            three = obs.at[1, 0, pl.ds(0, 3 * own), half(1 - d)]
            remote(three, three, y_send, y_recv.at[0], depth=1 - d).wait_recv()
        for k, b in enumerate((opp, left, right)):
            if q:
                over_depth(q, k, 1 - d).wait_recv()
            to_beside(q, b, 1 - d)

    def to_beside(q, b, h=None):
        for k, p, has, seam in sides:

            def send(part, **where):
                at = (rows(b), slice(None)) if part is None else (rows(b), half(part))
                remote(
                    obs.at[(1, q) + at], obs.at[(2 * k, q) + at], n_send.at[k], n_recv.at[q, k], region=p, **where
                ).start()

            @pl.when(jnp.logical_and(has, jnp.logical_not(seam)))
            def _():
                send(h)

            if h is None or h is d:

                @pl.when(seam)
                def _():
                    send(d)
                    send(d, depth=1 - d)

    def take_half(q):
        if not q:
            three = obs.at[1, 0, pl.ds(0, 3 * own), half(d)]
            remote(three, three, o_send, o_recv.at[0], member=opp).wait_recv()
        for k, b in enumerate((opp, left, right)):
            if q:
                o_copies(q)[k].wait_recv()
            to_depth(q, k)
            to_beside(q, b, d)

    def beside(q, w):
        k = w // 2
        return remote(obs.at[1, q], obs.at[w, q], n_send.at[k], n_recv.at[q, k], region=after)

    def has_window(w):
        return jnp.logical_and(r + w > 0, r + w < regions + 1)

    def small_copy(k, p):
        return remote(small.at[1], small.at[2 * k], s_send.at[k], s_recv.at[k], region=p)

    swap = remote(part.at[0], part.at[1], d_send, d_recv, depth=1 - d)

    for copy in o_copies(0):
        copy.start()
    send_ens(0, 1)
    with jax.named_scope("load_all"):
        for copy in loads[3:]:
            copy.wait()
    for copy in e_copies(1)[:EARLY]:
        copy.start()
    with jax.named_scope("pick"):
        spot_row = spots[...]
        picked = None
        for c in range(n_tile // CHUNK):
            at = pl.ds(c * CHUNK, CHUNK)
            index = lax.broadcasted_iota(jnp.int32, (CHUNK, n_obs), 0) + c * CHUNK
            hot = jnp.where(index == spot_row, 1.0, 0.0).astype(BF16)
            blend = wts[0] * ens[0, :, at].astype(F32)
            for l in range(1, n_var):
                blend = blend + wts[l] * ens[l, :, at].astype(F32)
            term = dot(blend.astype(BF16), hot)
            picked = term if picked is None else picked + term
        part[0] = picked.astype(BF16)
    swap.start()
    small[1, 0:1, :] = spot_row.astype(F32)
    for k, p, has, seam in sides:

        @pl.when(has)
        def _():
            small_copy(k, p).start()

    to_beside(0, j)

    def take_own(l, c):
        recv[l, rows(j), :] = ens[l, :, cols(j)]
        return c

    lax.fori_loop(0, n_var, take_own, 0)
    for l in range(first, n_var):
        recv[l + TWICE, rows(j), :] = ens[l, :, cols(left)]

    with jax.named_scope("swap"):
        swap.wait_recv()
    mixed = (part[0].astype(F32) + part[1].astype(F32)).astype(BF16)
    obs[1, 1, rows(j), :] = mixed
    mixed = mixed.astype(F32)
    part_sum = jnp.sum(mixed, axis=0, keepdims=True)
    apart = mixed - part_sum / own
    sums[j, 0:1, :] = part_sum
    sums[j, 1:2, :] = jnp.sum(apart * apart, axis=0, keepdims=True)
    m_copies = [
        remote(sums.at[j], sums.at[j], m_send, m_recv, member=p) for p in others
    ]
    for copy in m_copies + o_copies(1):
        copy.start()
    to_beside(1, j)
    for l in range(first, n_var):
        for copy in twice_copies(l):
            copy.start()
    for copy in e_copies(1)[EARLY:]:
        copy.start()
    send_ens(2, first)
    with jax.named_scope("noise_x"):
        take_half(0)

    with jax.named_scope("small"):
        for k, has in ((0, r > 0), (1, r < regions - 1)):

            @pl.when(has)
            def _():
                small_copy(k, after).wait_recv()

            @pl.when(jnp.logical_not(has))
            def _():
                small[2 * k] = jnp.ones_like(small[1])
                at = pl.ds(2 * k * n_obs, n_obs)
                anom_t[at, :] = jnp.zeros((n_obs, MEMBERS), BF16)
                gain[0, at, :] = jnp.zeros((n_obs, share), BF16)
                pert[:, at] = jnp.zeros((MEMBERS, n_obs), BF16)

    lane = lax.broadcasted_iota(jnp.int32, (n_obs, 128), 1)
    shifts = (
        jnp.where(r == 0, -16.0 * RADIUS, -RADIUS),
        jnp.float32(0.0),
        jnp.where(r == regions - 1, 16.0 * RADIUS, RADIUS),
    )
    with jax.named_scope("taper"):
        for w in range(3):
            spot = jnp.broadcast_to(small[w, 0:1, :] + shifts[w], (128, n_obs)).T
            for k, quarter in enumerate((j, left)):
                for c in range(share // 128):
                    tile = (lane + (quarter * share + c * 128)).astype(F32)
                    level = jnp.maximum(0.0, 1.0 - jnp.abs(tile - spot) / RADIUS)
                    taper[k, pl.ds(w * n_obs, n_obs), pl.ds(c * 128, 128)] = level * level / (MEMBERS - 1)

    with jax.named_scope("sums"):
        three_sums = sums.at[pl.ds(0, 3)]
        summed = remote(three_sums, three_sums, m_send, m_recv, member=opp)
        summed.wait_recv()
    mean = (sums[0, 0:1, :] + sums[1, 0:1, :] + sums[2, 0:1, :] + sums[3, 0:1, :]) / MEMBERS
    squares = jnp.zeros_like(mean)
    for p in range(peers):
        off = sums[p, 0:1, :] / own - mean
        squares = squares + (sums[p, 1:2, :] + own * off * off)
    spread = squares / (MEMBERS - 1)
    tot[1, 0:1, :] = mean
    tot[1, 1:2, :] = spread
    innovation = small[1, 1:2, :] - mean
    line = lax.broadcasted_iota(jnp.int32, (8, 128), 0)
    slots[0, z] = jnp.where(
        line < 4,
        jnp.sum(innovation * innovation, axis=1, keepdims=True),
        jnp.sum(spread + small[1, 2:3, :], axis=1, keepdims=True),
    )

    def tell(step, at, targets):
        for p in targets:
            remote(slots.at[step, at], slots.at[step, at], i_send.at[step], i_recv.at[step], region=p).start()

    def told(step):
        block = slots.at[step, pl.ds(0, 3)]
        return remote(block, block, i_send.at[step], i_recv.at[step], region=after)

    tell(0, z, ring_peers)
    with jax.named_scope("pred_x"):
        take_half(1)

    def tell_on():
        with jax.named_scope("told"):
            told(0).wait_recv()
            slots[1, 2 * y + core] = jnp.sum(slots[0], axis=0)
            tell(1, 2 * y + core, (r + other_core, across, across + other_core))

    pl.when(z == ring - 1)(tell_on)
    with jax.named_scope("noise_y"):
        from_depth(0)
    pl.when(z < ring - 1)(tell_on)
    def window(w):
        return pl.ds(pl.multiple_of(w * n_obs, n_obs), n_obs)

    def turned(w, mean):
        dev = obs[w, 1].astype(F32) - mean
        anom_t[window(w), :] = dev.astype(BF16).T
        return dev

    def stats(w):
        mean = jnp.sum(obs[w, 1].astype(F32), axis=0, keepdims=True) / MEMBERS
        dev = turned(w, mean)
        tot[w, 0:1, :] = mean
        tot[w, 1:2, :] = jnp.sum(dev * dev, axis=0, keepdims=True) / (MEMBERS - 1)

    def anomalies_of(l, slot):
        with jax.named_scope("take"):
            for count, here in ((3, l < first), (2, l >= first)):

                @pl.when(here)
                def _():
                    block = recv.at[l, pl.ds(0, count * own), :]
                    remote(block, block, e_send, e_recv.at[l], member=opp).wait_recv()

        state = recv[l].astype(F32)
        mean = jnp.sum(state, axis=0, keepdims=True) / MEMBERS
        means[slot, 0:1, :] = mean
        anoms[slot] = (state - mean).astype(BF16)

    def gain_of(slot, w, quarter=0):
        at = window(w)
        gain[slot, at, :] = (dot(anom_t[at, :], anoms[slot]) * taper[quarter, at, :]).astype(BF16)

    def perturbed(w, infl, root):
        mean, spread = tot[w, 0:1, :], tot[w, 1:2, :]
        factor = infl / (infl * spread + small[w, 2:3, :])
        innovation = small[w, 1:2, :] - mean
        dev = obs[w, 1].astype(F32) - mean
        moved = innovation + obs[w, 0].astype(F32) - root * dev
        pert[:, window(w)] = (moved * factor).astype(BF16)

    with jax.named_scope("anom0"):
        anomalies_of(0, 0)
    with jax.named_scope("pass"):
        for l in range(first, n_var):
            pass_on(l)
    with jax.named_scope("pred_y"):
        from_depth(1)
    with jax.named_scope("gain0"):
        turned(1, tot[1, 0:1, :])
        gain_of(0, 1)
    with jax.named_scope("near1"):
        beside(1, near).wait_recv()
    with jax.named_scope("gainn"):
        stats(near)
        gain_of(0, near)

    def far_gain():
        with jax.named_scope("far1"):
            beside(1, 2 - near).wait_recv()
        with jax.named_scope("gainf"):
            stats(2 - near)
            gain_of(0, 2 - near)

    has_far = has_window(2 - near)
    pl.when(jnp.logical_and(has_far, core == 0))(far_gain)
    with jax.named_scope("infl"):
        told(1).wait_recv()
    total = jnp.sum(slots[1], axis=0)
    infl = total[0:1, 0:1] / total[4:5, 0:1]
    root = jnp.sqrt(infl)
    infl_ref[...] = infl
    with jax.named_scope("pert1"):
        perturbed(1, infl, root)
    with jax.named_scope("near0"):
        beside(0, near).wait_recv()
    with jax.named_scope("pertn"):
        perturbed(near, infl, root)

    pl.when(jnp.logical_and(has_far, core == 1))(far_gain)

    @pl.when(has_far)
    def _():
        with jax.named_scope("far0"):
            beside(0, 2 - near).wait_recv()
        with jax.named_scope("pertf"):
            perturbed(2 - near, infl, root)

    def b_copies(l):
        return [
            remote(back.at[l, rows(p), :], out.at[l, :, cols(j)], b_send, b_recv, member=p)
            for k, p in enumerate(others)
        ]

    def analyse(l, c):
        slot = lax.rem(l, 2)
        with jax.named_scope("inc"):
            increment = dot(pert[...], gain[slot])
            back[l] = (means[slot, 0:1, :] + root * anoms[slot].astype(F32) + increment).astype(BF16)

        @pl.when(l < first)
        def _():
            for copy in b_copies(l):
                copy.start()
            out[l, :, cols(j)] = back[l, rows(j), :]

        for here, at, quarter, p in (
            (jnp.logical_and(l >= first, l < n_var), l, j, left),
            (l >= n_var, l - TWICE, left, right),
        ):

            @pl.when(here)
            def _():
                remote(back.at[l, rows(p), :], out.at[at, :, cols(quarter)], b_send, b_recv, member=p).start()
                out[at, :, cols(quarter)] = back[l, rows(j), :]

        @pl.when(l < n_var + TWICE - 1)
        def _():
            with jax.named_scope("gain"):
                anomalies_of(l + 1, 1 - slot)
                for w in range(3):
                    gain_of(1 - slot, w, (l + 1) // n_var)

        return c

    lax.fori_loop(0, n_var + TWICE, analyse, 0)

    with jax.named_scope("fin"):
        got = (3 * n_var - TWICE) * own
        deep = next(k for k in range(1, n_var) if got % (16 * k) == 0 and got // k <= peers * own)
        back_in = back.at[pl.ds(0, deep), pl.ds(0, got // deep), :]
        remote(back_in, back_in, b_send, b_recv, member=opp).wait_recv()

    with jax.named_scope("sent"):
        remote(back_in, back_in, b_send, b_recv, member=opp).wait_send()
        ens_in = recv.at[:, pl.ds(0, 3 * own), :]
        remote(ens_in, ens_in, e_send, e_recv.at[0], member=opp).wait_send()
        halves = obs.at[1, 0, pl.ds(0, 3 * own), :]
        remote(halves, halves, o_send, o_recv.at[0], member=opp).wait_send()
        remote(halves, halves, y_send, y_recv.at[0], depth=1 - d).wait_send()
        for k, p, has, seam in sides:

            @pl.when(has)
            def _():
                small_copy(k, after).wait_send()
                remote(obs.at[1], obs.at[2 * k], n_send.at[k], n_recv.at[0, k], region=after).wait_send()

        summed.wait_send()
        swap.wait_send()
        told(0).wait_send()
        told(1).wait_send()


def solution(mesh):
    regions, peers = mesh.shape["region"], mesh.shape["member"]

    def shards(ensemble, obs_weights, obs_tiles, obs_values, obs_error, obs_noise):
        n_var, own, n_tile = ensemble.shape
        n_obs = obs_tiles.shape[0]
        share, members = n_tile // peers, own * peers
        DMA = pltpu.SemaphoreType.DMA
        scratch = [
            pltpu.VMEM((n_var, own, n_tile), BF16),
            pltpu.SMEM((n_var,), F32),
            pltpu.VMEM((1, n_obs), jnp.int32),
            pltpu.VMEM((3, 8, n_obs), F32),
            pltpu.VMEM((own, n_obs), F32),
            pltpu.VMEM((2, own, n_obs), BF16),
            pltpu.VMEM((3, 2, members, n_obs), BF16),
            pltpu.VMEM((peers, 2, n_obs), F32),
            pltpu.VMEM((2, RING, 8, 128), F32),
            pltpu.VMEM((n_var + TWICE, members, share), BF16),
            pltpu.VMEM((n_var + TWICE, members, share), BF16),
            pltpu.VMEM((2, members, share), BF16),
            pltpu.VMEM((2, 8, share), F32),
            pltpu.VMEM((3 * n_obs, members), BF16),
            pltpu.VMEM((2, 3 * n_obs, share), F32),
            pltpu.VMEM((2, 3 * n_obs, share), BF16),
            pltpu.VMEM((members, 3 * n_obs), BF16),
            pltpu.VMEM((3, 8, n_obs), F32),
            DMA((7,)),
            DMA,
            DMA((n_var + 3 * TWICE,)),
            DMA,
            DMA,
            DMA,
            DMA((4,)),
            DMA,
            DMA((4,)),
            DMA((2,)),
            DMA((2, 2)),
            DMA((2,)),
            DMA((2,)),
            DMA,
            DMA,
            DMA,
            DMA,
            DMA((2,)),
            DMA((2,)),
        ]
        hbm = pl.BlockSpec(memory_space=pltpu.HBM)
        analysis, inflation = pl.pallas_call(
            lambda *refs: kernel(regions, peers, RING, *refs),
            out_shape=(
                pltpu.VMEM(ensemble.shape, BF16),
                pltpu.VMEM((1, 1), F32),
            ),
            in_specs=[hbm] * 6,
            out_specs=(pl.BlockSpec(memory_space=pltpu.VMEM), pl.BlockSpec(memory_space=pltpu.VMEM)),
            scratch_shapes=scratch,
            compiler_params=pltpu.CompilerParams(
                collective_id=0, has_side_effects=True, vmem_limit_bytes=56 * 2**20
            ),
        )(
            ensemble,
            obs_weights,
            obs_tiles.reshape(1, n_obs),
            obs_values.reshape(1, n_obs),
            obs_error.reshape(1, n_obs),
            obs_noise,
        )
        return analysis, inflation.reshape(())

    return jax.shard_map(
        shards,
        mesh=mesh,
        in_specs=(
            P("depth", "member", "region"),
            P("depth"),
            P("region"),
            P("region"),
            P("region"),
            P("member", "region"),
        ),
        out_specs=(P("depth", "member", "region"), P()),
        check_vma=False,
    )
```

```python
import jax
import jax.numpy as jnp
from jax import lax
from jax.experimental import pallas as pl
from jax.experimental.pallas import tpu as pltpu
from jax.sharding import PartitionSpec as P

MEMBERS = 384
RADIUS = 1024.0
RING = 4
CHUNK = 256
TWICE = 2
EARLY = (3, 1)
MESH = pl.DeviceIdType.MESH
F32 = jnp.float32
BF16 = jnp.bfloat16


def dot(a, b):
    return lax.dot_general(a, b, (((1,), (0,)), ((), ())), preferred_element_type=F32)


def kernel(
    regions,
    peers,
    ring,
    ens_hbm,
    wts_hbm,
    tiles_hbm,
    vals_hbm,
    err_hbm,
    noise_hbm,
    out,
    infl_ref,
    ens,
    wts,
    spots,
    small,
    noise,
    part,
    obs,
    sums,
    slots,
    recv,
    back,
    anoms,
    means,
    anom_t,
    taper,
    gain,
    pert,
    tot,
    load_sem,
    e_send,
    e_recv,
    b_send,
    b_recv,
    o_send,
    o_recv,
    y_send,
    y_recv,
    n_send,
    n_recv,
    s_send,
    s_recv,
    d_send,
    d_recv,
    m_send,
    m_recv,
    i_send,
    i_recv,
):
    n_var, own, n_tile = ens.shape
    n_obs = noise.shape[1]
    share = n_tile // peers
    r = lax.axis_index("region")
    d = lax.axis_index("depth")
    j = lax.axis_index("member")
    right, left, opp = lax.rem(j + 1, peers), lax.rem(j + 3, peers), lax.rem(j + 2, peers)
    after, before = lax.rem(r + 1, regions), lax.rem(r + regions - 1, regions)
    others = (opp, right, left)
    core, z, y = lax.rem(r, 2), lax.rem(r // 2, ring), r // (2 * ring)
    ring_peers = [r - 2 * z + 2 * lax.rem(z + o, ring) for o in range(1, ring)]
    across = r + 2 * ring * (1 - 2 * y)
    other_core = 1 - 2 * core
    sides = (
        (0, after, r < regions - 1, r == regions // 2 - 1),
        (1, before, r > 0, r == regions // 2),
    )
    near = 2 * lax.rem(r + 1, 2)

    def rows(b):
        return pl.ds(pl.multiple_of(b * own, 16), own)

    def cols(b):
        return pl.ds(pl.multiple_of(b * share, 128), share)

    def half(h):
        return pl.ds(pl.multiple_of(h * (n_obs // 2), 128), n_obs // 2)

    def remote(src, dst, send, rec, **where):
        return pltpu.make_async_remote_copy(src, dst, send, rec, device_id=where, device_id_type=MESH)

    barrier = pltpu.get_barrier_semaphore()

    def greet(**where):
        pl.semaphore_signal(barrier, inc=1, device_id=where, device_id_type=MESH)

    for p in others:
        greet(member=p)
    for p in ring_peers + [across, across + other_core]:
        greet(region=p)
    greet(depth=1 - d)
    for k, p, has, seam in sides:

        @pl.when(has)
        def _():
            greet(region=p)

        @pl.when(seam)
        def _():
            greet(region=p, depth=1 - d)

    greeted = ring + 5
    for k, p, has, seam in sides:
        greeted = greeted + has.astype(jnp.int32) + seam.astype(jnp.int32)

    rest = pl.ds(1, n_var - 1)
    loads = [
        pltpu.make_async_copy(err_hbm, small.at[1, pl.ds(2, 1)], load_sem.at[0]),
        pltpu.make_async_copy(noise_hbm, noise, load_sem.at[1]),
        pltpu.make_async_copy(ens_hbm.at[0], ens.at[0], load_sem.at[2]),
        pltpu.make_async_copy(tiles_hbm, spots, load_sem.at[3]),
        pltpu.make_async_copy(wts_hbm, wts, load_sem.at[4]),
        pltpu.make_async_copy(ens_hbm.at[rest], ens.at[rest], load_sem.at[5]),
        pltpu.make_async_copy(vals_hbm, small.at[1, pl.ds(1, 1)], load_sem.at[6]),
    ]
    for copy in loads:
        copy.start()

    with jax.named_scope("noise"):
        loads[0].wait()
        loads[1].wait()
        obs[1, 0, rows(j), :] = (jnp.sqrt(small[1, 2:3, :]) * noise[...]).astype(BF16)
    with jax.named_scope("ens"):
        loads[2].wait()
    with jax.named_scope("barrier"):
        pl.semaphore_wait(barrier, greeted)

    def e_copies(l):
        return [
            remote(ens.at[l, :, cols(p)], recv.at[l, rows(j), :], e_send, e_recv.at[l], member=p)
            for p in others
        ]

    def send_ens(first, last):
        def body(l, c):
            for copy in e_copies(l):
                copy.start()
            return c

        lax.fori_loop(first, last, body, 0)

    first = n_var - TWICE

    def twice_copies(l):
        far, rec = l + TWICE, n_var + TWICE + 2 * (l - first)
        return [
            remote(ens.at[l, :, cols(right)], recv.at[l, rows(j), :], e_send, e_recv.at[rec], member=right),
            remote(ens.at[l, :, cols(opp)], recv.at[far, rows(j), :], e_send, e_recv.at[rec + 1], member=left),
            remote(ens.at[l, :, cols(j)], recv.at[far, rows(j), :], e_send, e_recv.at[far], member=right),
            remote(ens.at[l, :, cols(left)], recv.at[l, rows(j), :], e_send, e_recv.at[l], member=left),
        ]

    def pass_on(l):
        far, copies = l + TWICE, twice_copies(l)
        block = recv.at[l, rows(left), :]
        copies[0].wait_recv()
        remote(block, recv.at[far, rows(left), :], e_send, e_recv.at[far], member=right).start()
        block = recv.at[far, rows(right), :]
        copies[1].wait_recv()
        remote(block, recv.at[l, rows(right), :], e_send, e_recv.at[l], member=left).start()

    def o_copies(q):
        block = obs.at[1, q, rows(j), half(d)]
        return [
            remote(block, block, o_send, o_recv.at[q * (1 + k)], member=p) for k, p in enumerate(others)
        ]

    def over_depth(q, k, h):
        block = obs.at[1, q, rows((opp, left, right)[k]), half(h)]
        return remote(block, block, y_send, y_recv.at[q * (1 + k)], depth=1 - d)

    def to_depth(q, k):
        over_depth(q, k, d).start()

    def from_depth(q):
        if not q:
            three = obs.at[1, 0, pl.ds(0, 3 * own), half(1 - d)]
            remote(three, three, y_send, y_recv.at[0], depth=1 - d).wait_recv()
        for k, b in enumerate((opp, left, right)):
            if q:
                over_depth(q, k, 1 - d).wait_recv()
            to_beside(q, b, 1 - d)

    def to_beside(q, b, h=None):
        for k, p, has, seam in sides:

            def send(part, **where):
                at = (rows(b), slice(None)) if part is None else (rows(b), half(part))
                remote(
                    obs.at[(1, q) + at], obs.at[(2 * k, q) + at], n_send.at[k], n_recv.at[q, k], region=p, **where
                ).start()

            @pl.when(jnp.logical_and(has, jnp.logical_not(seam)))
            def _():
                send(h)

            if h is None or h is d:

                @pl.when(seam)
                def _():
                    send(d)
                    send(d, depth=1 - d)

    def take_half(q):
        if not q:
            three = obs.at[1, 0, pl.ds(0, 3 * own), half(d)]
            remote(three, three, o_send, o_recv.at[0], member=opp).wait_recv()
        for k, b in enumerate((opp, left, right)):
            if q:
                o_copies(q)[k].wait_recv()
            to_depth(q, k)
            to_beside(q, b, d)

    def beside(q, w):
        k = w // 2
        return remote(obs.at[1, q], obs.at[w, q], n_send.at[k], n_recv.at[q, k], region=after)

    def has_window(w):
        return jnp.logical_and(r + w > 0, r + w < regions + 1)

    def small_copy(k, p):
        return remote(small.at[1], small.at[2 * k], s_send.at[k], s_recv.at[k], region=p)

    swap = remote(part.at[0], part.at[1], d_send, d_recv, depth=1 - d)

    for copy in o_copies(0):
        copy.start()
    send_ens(0, 1)
    with jax.named_scope("load_all"):
        for copy in loads[3:]:
            copy.wait()
    for h, count in enumerate(EARLY):

        @pl.when(d == h)
        def _():
            for copy in e_copies(1)[:count]:
                copy.start()

    with jax.named_scope("pick"):
        spot_row = spots[...]
        picked = None
        for c in range(n_tile // CHUNK):
            at = pl.ds(c * CHUNK, CHUNK)
            index = lax.broadcasted_iota(jnp.int32, (CHUNK, n_obs), 0) + c * CHUNK
            hot = jnp.where(index == spot_row, 1.0, 0.0).astype(BF16)
            blend = wts[0] * ens[0, :, at].astype(F32)
            for l in range(1, n_var):
                blend = blend + wts[l] * ens[l, :, at].astype(F32)
            term = dot(blend.astype(BF16), hot)
            picked = term if picked is None else picked + term
        part[0] = picked.astype(BF16)
    swap.start()
    small[1, 0:1, :] = spot_row.astype(F32)
    for k, p, has, seam in sides:

        @pl.when(has)
        def _():
            small_copy(k, p).start()

    to_beside(0, j)

    def take_own(l, c):
        recv[l, rows(j), :] = ens[l, :, cols(j)]
        return c

    lax.fori_loop(0, n_var, take_own, 0)
    for l in range(first, n_var):
        recv[l + TWICE, rows(j), :] = ens[l, :, cols(left)]

    with jax.named_scope("swap"):
        swap.wait_recv()
    mixed = (part[0].astype(F32) + part[1].astype(F32)).astype(BF16)
    obs[1, 1, rows(j), :] = mixed
    mixed = mixed.astype(F32)
    part_sum = jnp.sum(mixed, axis=0, keepdims=True)
    apart = mixed - part_sum / own
    sums[j, 0:1, :] = part_sum
    sums[j, 1:2, :] = jnp.sum(apart * apart, axis=0, keepdims=True)
    m_copies = [
        remote(sums.at[j], sums.at[j], m_send, m_recv, member=p) for p in others
    ]
    for copy in m_copies + o_copies(1):
        copy.start()
    to_beside(1, j)
    for l in range(first, n_var):
        for copy in twice_copies(l):
            copy.start()
    for h, count in enumerate(EARLY):

        @pl.when(d == h)
        def _():
            for copy in e_copies(1)[count:]:
                copy.start()

    send_ens(2, first)
    with jax.named_scope("noise_x"):
        take_half(0)

    with jax.named_scope("small"):
        for k, has in ((0, r > 0), (1, r < regions - 1)):

            @pl.when(has)
            def _():
                small_copy(k, after).wait_recv()

            @pl.when(jnp.logical_not(has))
            def _():
                small[2 * k] = jnp.ones_like(small[1])
                at = pl.ds(2 * k * n_obs, n_obs)
                anom_t[at, :] = jnp.zeros((n_obs, MEMBERS), BF16)
                gain[0, at, :] = jnp.zeros((n_obs, share), BF16)
                pert[:, at] = jnp.zeros((MEMBERS, n_obs), BF16)

    lane = lax.broadcasted_iota(jnp.int32, (n_obs, 128), 1)
    shifts = (
        jnp.where(r == 0, -16.0 * RADIUS, -RADIUS),
        jnp.float32(0.0),
        jnp.where(r == regions - 1, 16.0 * RADIUS, RADIUS),
    )
    with jax.named_scope("taper"):
        for w in range(3):
            spot = jnp.broadcast_to(small[w, 0:1, :] + shifts[w], (128, n_obs)).T
            for k, quarter in enumerate((j, left)):
                for c in range(share // 128):
                    tile = (lane + (quarter * share + c * 128)).astype(F32)
                    level = jnp.maximum(0.0, 1.0 - jnp.abs(tile - spot) / RADIUS)
                    taper[k, pl.ds(w * n_obs, n_obs), pl.ds(c * 128, 128)] = level * level / (MEMBERS - 1)

    with jax.named_scope("sums"):
        three_sums = sums.at[pl.ds(0, 3)]
        summed = remote(three_sums, three_sums, m_send, m_recv, member=opp)
        summed.wait_recv()
    mean = (sums[0, 0:1, :] + sums[1, 0:1, :] + sums[2, 0:1, :] + sums[3, 0:1, :]) / MEMBERS
    squares = jnp.zeros_like(mean)
    for p in range(peers):
        off = sums[p, 0:1, :] / own - mean
        squares = squares + (sums[p, 1:2, :] + own * off * off)
    spread = squares / (MEMBERS - 1)
    tot[1, 0:1, :] = mean
    tot[1, 1:2, :] = spread
    innovation = small[1, 1:2, :] - mean
    line = lax.broadcasted_iota(jnp.int32, (8, 128), 0)
    slots[0, z] = jnp.where(
        line < 4,
        jnp.sum(innovation * innovation, axis=1, keepdims=True),
        jnp.sum(spread + small[1, 2:3, :], axis=1, keepdims=True),
    )

    def tell(step, at, targets):
        for p in targets:
            remote(slots.at[step, at], slots.at[step, at], i_send.at[step], i_recv.at[step], region=p).start()

    def told(step):
        block = slots.at[step, pl.ds(0, 3)]
        return remote(block, block, i_send.at[step], i_recv.at[step], region=after)

    tell(0, z, ring_peers)
    with jax.named_scope("pred_x"):
        take_half(1)

    def tell_on():
        with jax.named_scope("told"):
            told(0).wait_recv()
            slots[1, 2 * y + core] = jnp.sum(slots[0], axis=0)
            tell(1, 2 * y + core, (r + other_core, across, across + other_core))

    pl.when(z == ring - 1)(tell_on)
    with jax.named_scope("noise_y"):
        from_depth(0)
    pl.when(z < ring - 1)(tell_on)
    def window(w):
        return pl.ds(pl.multiple_of(w * n_obs, n_obs), n_obs)

    def turned(w, mean):
        dev = obs[w, 1].astype(F32) - mean
        anom_t[window(w), :] = dev.astype(BF16).T
        return dev

    def stats(w):
        mean = jnp.sum(obs[w, 1].astype(F32), axis=0, keepdims=True) / MEMBERS
        dev = turned(w, mean)
        tot[w, 0:1, :] = mean
        tot[w, 1:2, :] = jnp.sum(dev * dev, axis=0, keepdims=True) / (MEMBERS - 1)

    def anomalies_of(l, slot):
        with jax.named_scope("take"):
            for count, here in ((3, l < first), (2, l >= first)):

                @pl.when(here)
                def _():
                    block = recv.at[l, pl.ds(0, count * own), :]
                    remote(block, block, e_send, e_recv.at[l], member=opp).wait_recv()

        state = recv[l].astype(F32)
        mean = jnp.sum(state, axis=0, keepdims=True) / MEMBERS
        means[slot, 0:1, :] = mean
        anoms[slot] = (state - mean).astype(BF16)

    def gain_of(slot, w, quarter=0):
        at = window(w)
        gain[slot, at, :] = (dot(anom_t[at, :], anoms[slot]) * taper[quarter, at, :]).astype(BF16)

    def perturbed(w, infl, root):
        mean, spread = tot[w, 0:1, :], tot[w, 1:2, :]
        factor = infl / (infl * spread + small[w, 2:3, :])
        innovation = small[w, 1:2, :] - mean
        dev = obs[w, 1].astype(F32) - mean
        moved = innovation + obs[w, 0].astype(F32) - root * dev
        pert[:, window(w)] = (moved * factor).astype(BF16)

    with jax.named_scope("anom0"):
        anomalies_of(0, 0)
    with jax.named_scope("pred_y"):
        from_depth(1)
    with jax.named_scope("pass"):
        for l in range(first, n_var):
            pass_on(l)
    with jax.named_scope("gain0"):
        turned(1, tot[1, 0:1, :])
        gain_of(0, 1)
    with jax.named_scope("near1"):
        beside(1, near).wait_recv()
    with jax.named_scope("gainn"):
        stats(near)
        gain_of(0, near)

    def far_gain():
        with jax.named_scope("far1"):
            beside(1, 2 - near).wait_recv()
        with jax.named_scope("gainf"):
            stats(2 - near)
            gain_of(0, 2 - near)

    has_far = has_window(2 - near)
    pl.when(jnp.logical_and(has_far, core == 0))(far_gain)
    with jax.named_scope("infl"):
        told(1).wait_recv()
    total = jnp.sum(slots[1], axis=0)
    infl = total[0:1, 0:1] / total[4:5, 0:1]
    root = jnp.sqrt(infl)
    infl_ref[...] = infl
    with jax.named_scope("pert1"):
        perturbed(1, infl, root)
    with jax.named_scope("near0"):
        beside(0, near).wait_recv()
    with jax.named_scope("pertn"):
        perturbed(near, infl, root)

    pl.when(jnp.logical_and(has_far, core == 1))(far_gain)

    @pl.when(has_far)
    def _():
        with jax.named_scope("far0"):
            beside(0, 2 - near).wait_recv()
        with jax.named_scope("pertf"):
            perturbed(2 - near, infl, root)

    def b_copies(l):
        return [
            remote(back.at[l, rows(p), :], out.at[l, :, cols(j)], b_send, b_recv, member=p)
            for k, p in enumerate(others)
        ]

    def analyse(l, c):
        slot = lax.rem(l, 2)
        with jax.named_scope("inc"):
            increment = dot(pert[...], gain[slot])
            back[l] = (means[slot, 0:1, :] + root * anoms[slot].astype(F32) + increment).astype(BF16)

        @pl.when(l < first)
        def _():
            for copy in b_copies(l):
                copy.start()
            out[l, :, cols(j)] = back[l, rows(j), :]

        for here, at, quarter, p in (
            (jnp.logical_and(l >= first, l < n_var), l, j, left),
            (l >= n_var, l - TWICE, left, right),
        ):

            @pl.when(here)
            def _():
                remote(back.at[l, rows(p), :], out.at[at, :, cols(quarter)], b_send, b_recv, member=p).start()
                out[at, :, cols(quarter)] = back[l, rows(j), :]

        @pl.when(l < n_var + TWICE - 1)
        def _():
            with jax.named_scope("gain"):
                anomalies_of(l + 1, 1 - slot)
                for w in range(3):
                    gain_of(1 - slot, w, (l + 1) // n_var)

        return c

    lax.fori_loop(0, n_var + TWICE, analyse, 0)

    with jax.named_scope("fin"):
        got = (3 * n_var - TWICE) * own
        deep = next(k for k in range(1, n_var) if got % (16 * k) == 0 and got // k <= peers * own)
        back_in = back.at[pl.ds(0, deep), pl.ds(0, got // deep), :]
        remote(back_in, back_in, b_send, b_recv, member=opp).wait_recv()

    with jax.named_scope("sent"):
        remote(back_in, back_in, b_send, b_recv, member=opp).wait_send()
        ens_in = recv.at[:, pl.ds(0, 3 * own), :]
        remote(ens_in, ens_in, e_send, e_recv.at[0], member=opp).wait_send()
        halves = obs.at[1, 0, pl.ds(0, 3 * own), :]
        remote(halves, halves, o_send, o_recv.at[0], member=opp).wait_send()
        remote(halves, halves, y_send, y_recv.at[0], depth=1 - d).wait_send()
        for k, p, has, seam in sides:

            @pl.when(has)
            def _():
                small_copy(k, after).wait_send()
                remote(obs.at[1], obs.at[2 * k], n_send.at[k], n_recv.at[0, k], region=after).wait_send()

        summed.wait_send()
        swap.wait_send()
        told(0).wait_send()
        told(1).wait_send()


def solution(mesh):
    regions, peers = mesh.shape["region"], mesh.shape["member"]

    def shards(ensemble, obs_weights, obs_tiles, obs_values, obs_error, obs_noise):
        n_var, own, n_tile = ensemble.shape
        n_obs = obs_tiles.shape[0]
        share, members = n_tile // peers, own * peers
        DMA = pltpu.SemaphoreType.DMA
        scratch = [
            pltpu.VMEM((n_var, own, n_tile), BF16),
            pltpu.SMEM((n_var,), F32),
            pltpu.VMEM((1, n_obs), jnp.int32),
            pltpu.VMEM((3, 8, n_obs), F32),
            pltpu.VMEM((own, n_obs), F32),
            pltpu.VMEM((2, own, n_obs), BF16),
            pltpu.VMEM((3, 2, members, n_obs), BF16),
            pltpu.VMEM((peers, 2, n_obs), F32),
            pltpu.VMEM((2, RING, 8, 128), F32),
            pltpu.VMEM((n_var + TWICE, members, share), BF16),
            pltpu.VMEM((n_var + TWICE, members, share), BF16),
            pltpu.VMEM((2, members, share), BF16),
            pltpu.VMEM((2, 8, share), F32),
            pltpu.VMEM((3 * n_obs, members), BF16),
            pltpu.VMEM((2, 3 * n_obs, share), F32),
            pltpu.VMEM((2, 3 * n_obs, share), BF16),
            pltpu.VMEM((members, 3 * n_obs), BF16),
            pltpu.VMEM((3, 8, n_obs), F32),
            DMA((7,)),
            DMA,
            DMA((n_var + 3 * TWICE,)),
            DMA,
            DMA,
            DMA,
            DMA((4,)),
            DMA,
            DMA((4,)),
            DMA((2,)),
            DMA((2, 2)),
            DMA((2,)),
            DMA((2,)),
            DMA,
            DMA,
            DMA,
            DMA,
            DMA((2,)),
            DMA((2,)),
        ]
        hbm = pl.BlockSpec(memory_space=pltpu.HBM)
        analysis, inflation = pl.pallas_call(
            lambda *refs: kernel(regions, peers, RING, *refs),
            out_shape=(
                pltpu.VMEM(ensemble.shape, BF16),
                pltpu.VMEM((1, 1), F32),
            ),
            in_specs=[hbm] * 6,
            out_specs=(pl.BlockSpec(memory_space=pltpu.VMEM), pl.BlockSpec(memory_space=pltpu.VMEM)),
            scratch_shapes=scratch,
            compiler_params=pltpu.CompilerParams(
                collective_id=0, has_side_effects=True, vmem_limit_bytes=56 * 2**20
            ),
        )(
            ensemble,
            obs_weights,
            obs_tiles.reshape(1, n_obs),
            obs_values.reshape(1, n_obs),
            obs_error.reshape(1, n_obs),
            obs_noise,
        )
        return analysis, inflation.reshape(())

    return jax.shard_map(
        shards,
        mesh=mesh,
        in_specs=(
            P("depth", "member", "region"),
            P("depth"),
            P("region"),
            P("region"),
            P("region"),
            P("member", "region"),
        ),
        out_specs=(P("depth", "member", "region"), P()),
        check_vma=False,
    )
```

```python
import jax
import jax.numpy as jnp
from jax import lax
from jax.experimental import pallas as pl
from jax.experimental.pallas import tpu as pltpu
from jax.sharding import PartitionSpec as P

MEMBERS = 384
RADIUS = 1024.0
RING = 4
CHUNK = 256
TWICE = 2
EARLY = (3, 1)
MESH = pl.DeviceIdType.MESH
F32 = jnp.float32
BF16 = jnp.bfloat16


def dot(a, b):
    return lax.dot_general(a, b, (((1,), (0,)), ((), ())), preferred_element_type=F32)


def kernel(
    regions,
    peers,
    ring,
    ens_hbm,
    wts_hbm,
    tiles_hbm,
    vals_hbm,
    err_hbm,
    noise_hbm,
    out,
    infl_ref,
    ens,
    wts,
    spots,
    small,
    noise,
    part,
    obs,
    sums,
    slots,
    recv,
    back,
    anoms,
    means,
    anom_t,
    taper,
    gain,
    pert,
    tot,
    load_sem,
    e_send,
    e_recv,
    b_send,
    b_recv,
    o_send,
    o_recv,
    y_send,
    y_recv,
    n_send,
    n_recv,
    s_send,
    s_recv,
    d_send,
    d_recv,
    m_send,
    m_recv,
    i_send,
    i_recv,
):
    n_var, own, n_tile = ens.shape
    n_obs = noise.shape[1]
    share = n_tile // peers
    r = lax.axis_index("region")
    d = lax.axis_index("depth")
    j = lax.axis_index("member")
    right, left, opp = lax.rem(j + 1, peers), lax.rem(j + 3, peers), lax.rem(j + 2, peers)
    after, before = lax.rem(r + 1, regions), lax.rem(r + regions - 1, regions)
    others = (opp, right, left)
    core, z, y = lax.rem(r, 2), lax.rem(r // 2, ring), r // (2 * ring)
    ring_peers = [r - 2 * z + 2 * lax.rem(z + o, ring) for o in range(1, ring)]
    across = r + 2 * ring * (1 - 2 * y)
    other_core = 1 - 2 * core
    sides = (
        (0, after, r < regions - 1, r == regions // 2 - 1),
        (1, before, r > 0, r == regions // 2),
    )
    near = 2 * lax.rem(r + 1, 2)

    def rows(b):
        return pl.ds(pl.multiple_of(b * own, 16), own)

    def cols(b):
        return pl.ds(pl.multiple_of(b * share, 128), share)

    def half(h):
        return pl.ds(pl.multiple_of(h * (n_obs // 2), 128), n_obs // 2)

    def remote(src, dst, send, rec, **where):
        return pltpu.make_async_remote_copy(src, dst, send, rec, device_id=where, device_id_type=MESH)

    barrier = pltpu.get_barrier_semaphore()

    def greet(**where):
        pl.semaphore_signal(barrier, inc=1, device_id=where, device_id_type=MESH)

    for p in others:
        greet(member=p)
    for p in ring_peers + [across, across + other_core]:
        greet(region=p)
    greet(depth=1 - d)
    for k, p, has, seam in sides:

        @pl.when(has)
        def _():
            greet(region=p)

        @pl.when(seam)
        def _():
            greet(region=p, depth=1 - d)

    greeted = ring + 5
    for k, p, has, seam in sides:
        greeted = greeted + has.astype(jnp.int32) + seam.astype(jnp.int32)

    rest = pl.ds(1, n_var - 1)
    loads = [
        pltpu.make_async_copy(err_hbm, small.at[1, pl.ds(2, 1)], load_sem.at[0]),
        pltpu.make_async_copy(noise_hbm, noise, load_sem.at[1]),
        pltpu.make_async_copy(ens_hbm.at[0], ens.at[0], load_sem.at[2]),
        pltpu.make_async_copy(tiles_hbm, spots, load_sem.at[3]),
        pltpu.make_async_copy(wts_hbm, wts, load_sem.at[4]),
        pltpu.make_async_copy(ens_hbm.at[rest], ens.at[rest], load_sem.at[5]),
        pltpu.make_async_copy(vals_hbm, small.at[1, pl.ds(1, 1)], load_sem.at[6]),
    ]
    for copy in loads:
        copy.start()

    with jax.named_scope("noise"):
        loads[0].wait()
        loads[1].wait()
        obs[1, 0, rows(j), :] = (jnp.sqrt(small[1, 2:3, :]) * noise[...]).astype(BF16)
    with jax.named_scope("ens"):
        loads[2].wait()
    with jax.named_scope("barrier"):
        pl.semaphore_wait(barrier, greeted)

    def e_copies(l):
        return [
            remote(ens.at[l, :, cols(p)], recv.at[l, rows(j), :], e_send, e_recv.at[l], member=p)
            for p in others
        ]

    def send_ens(first, last):
        def body(l, c):
            for copy in e_copies(l):
                copy.start()
            return c

        lax.fori_loop(first, last, body, 0)

    first = n_var - TWICE

    def twice_copies(l):
        far, rec = l + TWICE, n_var + TWICE + 2 * (l - first)
        return [
            remote(ens.at[l, :, cols(right)], recv.at[l, rows(j), :], e_send, e_recv.at[rec], member=right),
            remote(ens.at[l, :, cols(opp)], recv.at[far, rows(j), :], e_send, e_recv.at[rec + 1], member=left),
            remote(ens.at[l, :, cols(j)], recv.at[far, rows(j), :], e_send, e_recv.at[far], member=right),
            remote(ens.at[l, :, cols(left)], recv.at[l, rows(j), :], e_send, e_recv.at[l], member=left),
        ]

    def pass_on(l):
        far, copies = l + TWICE, twice_copies(l)
        block = recv.at[l, rows(left), :]
        copies[0].wait_recv()
        remote(block, recv.at[far, rows(left), :], e_send, e_recv.at[far], member=right).start()
        block = recv.at[far, rows(right), :]
        copies[1].wait_recv()
        remote(block, recv.at[l, rows(right), :], e_send, e_recv.at[l], member=left).start()

    def o_copies(q):
        block = obs.at[1, q, rows(j), half(d)]
        return [
            remote(block, block, o_send, o_recv.at[q * (1 + k)], member=p) for k, p in enumerate(others)
        ]

    def over_depth(q, k, h):
        block = obs.at[1, q, rows((opp, left, right)[k]), half(h)]
        return remote(block, block, y_send, y_recv.at[q * (1 + k)], depth=1 - d)

    def to_depth(q, k):
        over_depth(q, k, d).start()

    def from_depth(q):
        if not q:
            three = obs.at[1, 0, pl.ds(0, 3 * own), half(1 - d)]
            remote(three, three, y_send, y_recv.at[0], depth=1 - d).wait_recv()
        for k, b in enumerate((opp, left, right)):
            if q:
                over_depth(q, k, 1 - d).wait_recv()
            to_beside(q, b, 1 - d)

    def to_beside(q, b, h=None):
        for k, p, has, seam in sides:

            def send(part, **where):
                at = (rows(b), slice(None)) if part is None else (rows(b), half(part))
                remote(
                    obs.at[(1, q) + at], obs.at[(2 * k, q) + at], n_send.at[k], n_recv.at[q, k], region=p, **where
                ).start()

            @pl.when(jnp.logical_and(has, jnp.logical_not(seam)))
            def _():
                send(h)

            if h is None or h is d:

                @pl.when(seam)
                def _():
                    send(d)
                    send(d, depth=1 - d)

    def take_half(q):
        if not q:
            three = obs.at[1, 0, pl.ds(0, 3 * own), half(d)]
            remote(three, three, o_send, o_recv.at[0], member=opp).wait_recv()
        for k, b in enumerate((opp, left, right)):
            if q:
                o_copies(q)[k].wait_recv()
            to_depth(q, k)
            to_beside(q, b, d)

    def beside(q, w):
        k = w // 2
        return remote(obs.at[1, q], obs.at[w, q], n_send.at[k], n_recv.at[q, k], region=after)

    def has_window(w):
        return jnp.logical_and(r + w > 0, r + w < regions + 1)

    def small_copy(k, p):
        return remote(small.at[1], small.at[2 * k], s_send.at[k], s_recv.at[k], region=p)

    swap = remote(part.at[0], part.at[1], d_send, d_recv, depth=1 - d)

    for copy in o_copies(0):
        copy.start()
    send_ens(0, 1)
    with jax.named_scope("load_all"):
        for copy in loads[3:]:
            copy.wait()
    for h, count in enumerate(EARLY):

        @pl.when(d == h)
        def _():
            for copy in e_copies(1)[:count]:
                copy.start()

    with jax.named_scope("pick"):
        spot_row = spots[...]
        picked = None
        for c in range(n_tile // CHUNK):
            at = pl.ds(c * CHUNK, CHUNK)
            index = lax.broadcasted_iota(jnp.int32, (CHUNK, n_obs), 0) + c * CHUNK
            hot = jnp.where(index == spot_row, 1.0, 0.0).astype(BF16)
            blend = wts[0] * ens[0, :, at].astype(F32)
            for l in range(1, n_var):
                blend = blend + wts[l] * ens[l, :, at].astype(F32)
            term = dot(blend.astype(BF16), hot)
            picked = term if picked is None else picked + term
        part[0] = picked.astype(BF16)
    swap.start()
    small[1, 0:1, :] = spot_row.astype(F32)
    for k, p, has, seam in sides:

        @pl.when(has)
        def _():
            small_copy(k, p).start()

    to_beside(0, j)

    def take_own(l, c):
        recv[l, rows(j), :] = ens[l, :, cols(j)]
        return c

    lax.fori_loop(0, n_var, take_own, 0)
    for l in range(first, n_var):
        recv[l + TWICE, rows(j), :] = ens[l, :, cols(left)]

    with jax.named_scope("swap"):
        swap.wait_recv()
    mixed = (part[0].astype(F32) + part[1].astype(F32)).astype(BF16)
    obs[1, 1, rows(j), :] = mixed
    mixed = mixed.astype(F32)
    part_sum = jnp.sum(mixed, axis=0, keepdims=True)
    apart = mixed - part_sum / own
    sums[j, 0:1, :] = part_sum
    sums[j, 1:2, :] = jnp.sum(apart * apart, axis=0, keepdims=True)
    m_copies = [
        remote(sums.at[j], sums.at[j], m_send, m_recv, member=p) for p in others
    ]
    for copy in m_copies + o_copies(1):
        copy.start()
    to_beside(1, j)
    for l in range(first, n_var):
        for copy in twice_copies(l):
            copy.start()
    for h, count in enumerate(EARLY):

        @pl.when(d == h)
        def _():
            for copy in e_copies(1)[count:]:
                copy.start()

    send_ens(2, first)
    with jax.named_scope("noise_x"):
        take_half(0)

    with jax.named_scope("small"):
        for k, has in ((0, r > 0), (1, r < regions - 1)):

            @pl.when(has)
            def _():
                small_copy(k, after).wait_recv()

            @pl.when(jnp.logical_not(has))
            def _():
                small[2 * k] = jnp.ones_like(small[1])
                at = pl.ds(2 * k * n_obs, n_obs)
                anom_t[at, :] = jnp.zeros((n_obs, MEMBERS), BF16)
                gain[0, at, :] = jnp.zeros((n_obs, share), BF16)
                pert[:, at] = jnp.zeros((MEMBERS, n_obs), BF16)

    lane = lax.broadcasted_iota(jnp.int32, (n_obs, 128), 1)
    shifts = (
        jnp.where(r == 0, -16.0 * RADIUS, -RADIUS),
        jnp.float32(0.0),
        jnp.where(r == regions - 1, 16.0 * RADIUS, RADIUS),
    )
    with jax.named_scope("taper"):
        for w in range(3):
            spot = jnp.broadcast_to(small[w, 0:1, :] + shifts[w], (128, n_obs)).T
            for k, quarter in enumerate((j, left)):
                for c in range(share // 128):
                    tile = (lane + (quarter * share + c * 128)).astype(F32)
                    level = jnp.maximum(0.0, 1.0 - jnp.abs(tile - spot) / RADIUS)
                    taper[k, pl.ds(w * n_obs, n_obs), pl.ds(c * 128, 128)] = level * level / (MEMBERS - 1)

    with jax.named_scope("sums"):
        three_sums = sums.at[pl.ds(0, 3)]
        summed = remote(three_sums, three_sums, m_send, m_recv, member=opp)
        summed.wait_recv()
    mean = (sums[0, 0:1, :] + sums[1, 0:1, :] + sums[2, 0:1, :] + sums[3, 0:1, :]) / MEMBERS
    squares = jnp.zeros_like(mean)
    for p in range(peers):
        off = sums[p, 0:1, :] / own - mean
        squares = squares + (sums[p, 1:2, :] + own * off * off)
    spread = squares / (MEMBERS - 1)
    tot[1, 0:1, :] = mean
    tot[1, 1:2, :] = spread
    innovation = small[1, 1:2, :] - mean
    line = lax.broadcasted_iota(jnp.int32, (8, 128), 0)
    slots[0, z] = jnp.where(
        line < 4,
        jnp.sum(innovation * innovation, axis=1, keepdims=True),
        jnp.sum(spread + small[1, 2:3, :], axis=1, keepdims=True),
    )

    def tell(step, at, targets):
        for p in targets:
            remote(slots.at[step, at], slots.at[step, at], i_send.at[step], i_recv.at[step], region=p).start()

    def told(step):
        block = slots.at[step, pl.ds(0, 3)]
        return remote(block, block, i_send.at[step], i_recv.at[step], region=after)

    tell(0, z, ring_peers)
    with jax.named_scope("pred_x"):
        take_half(1)

    def tell_on():
        with jax.named_scope("told"):
            told(0).wait_recv()
            slots[1, 2 * y + core] = jnp.sum(slots[0], axis=0)
            tell(1, 2 * y + core, (r + other_core, across, across + other_core))

    pl.when(z == ring - 1)(tell_on)
    with jax.named_scope("noise_y"):
        from_depth(0)
    pl.when(z < ring - 1)(tell_on)
    def window(w):
        return pl.ds(pl.multiple_of(w * n_obs, n_obs), n_obs)

    def turned(w, mean):
        dev = obs[w, 1].astype(F32) - mean
        anom_t[window(w), :] = dev.astype(BF16).T
        return dev

    def stats(w):
        mean = jnp.sum(obs[w, 1].astype(F32), axis=0, keepdims=True) / MEMBERS
        dev = turned(w, mean)
        tot[w, 0:1, :] = mean
        tot[w, 1:2, :] = jnp.sum(dev * dev, axis=0, keepdims=True) / (MEMBERS - 1)

    def anomalies_of(l, slot):
        with jax.named_scope("take"):
            for count, here in ((3, l < first), (2, l >= first)):

                @pl.when(here)
                def _():
                    block = recv.at[l, pl.ds(0, count * own), :]
                    remote(block, block, e_send, e_recv.at[l], member=opp).wait_recv()

        state = recv[l].astype(F32)
        mean = jnp.sum(state, axis=0, keepdims=True) / MEMBERS
        means[slot, 0:1, :] = mean
        anoms[slot] = (state - mean).astype(BF16)

    def gain_of(slot, w, quarter=0):
        at = window(w)
        gain[slot, at, :] = (dot(anom_t[at, :], anoms[slot]) * taper[quarter, at, :]).astype(BF16)

    def perturbed(w, infl, root):
        mean, spread = tot[w, 0:1, :], tot[w, 1:2, :]
        factor = infl / (infl * spread + small[w, 2:3, :])
        innovation = small[w, 1:2, :] - mean
        dev = obs[w, 1].astype(F32) - mean
        moved = innovation + obs[w, 0].astype(F32) - root * dev
        pert[:, window(w)] = (moved * factor).astype(BF16)

    with jax.named_scope("anom0"):
        anomalies_of(0, 0)
    with jax.named_scope("pred_y"):
        from_depth(1)
    with jax.named_scope("pass"):
        for l in range(first, n_var):
            pass_on(l)
    with jax.named_scope("gain0"):
        turned(1, tot[1, 0:1, :])
        gain_of(0, 1)
    def near_gain():
        with jax.named_scope("near1"):
            beside(1, near).wait_recv()
        with jax.named_scope("gainn"):
            stats(near)
            gain_of(0, near)

    pl.when(core == 0)(near_gain)

    def far_gain():
        with jax.named_scope("far1"):
            beside(1, 2 - near).wait_recv()
        with jax.named_scope("gainf"):
            stats(2 - near)
            gain_of(0, 2 - near)

    has_far = has_window(2 - near)
    pl.when(jnp.logical_and(has_far, core == 0))(far_gain)
    with jax.named_scope("infl"):
        told(1).wait_recv()
    total = jnp.sum(slots[1], axis=0)
    infl = total[0:1, 0:1] / total[4:5, 0:1]
    root = jnp.sqrt(infl)
    infl_ref[...] = infl
    with jax.named_scope("pert1"):
        perturbed(1, infl, root)
    pl.when(core == 1)(near_gain)
    with jax.named_scope("near0"):
        beside(0, near).wait_recv()
    with jax.named_scope("pertn"):
        perturbed(near, infl, root)

    pl.when(jnp.logical_and(has_far, core == 1))(far_gain)

    @pl.when(has_far)
    def _():
        with jax.named_scope("far0"):
            beside(0, 2 - near).wait_recv()
        with jax.named_scope("pertf"):
            perturbed(2 - near, infl, root)

    def b_copies(l):
        return [
            remote(back.at[l, rows(p), :], out.at[l, :, cols(j)], b_send, b_recv, member=p)
            for k, p in enumerate(others)
        ]

    def analyse(l, c):
        slot = lax.rem(l, 2)
        with jax.named_scope("inc"):
            increment = dot(pert[...], gain[slot])
            back[l] = (means[slot, 0:1, :] + root * anoms[slot].astype(F32) + increment).astype(BF16)

        @pl.when(l < first)
        def _():
            for copy in b_copies(l):
                copy.start()
            out[l, :, cols(j)] = back[l, rows(j), :]

        for here, at, quarter, p in (
            (jnp.logical_and(l >= first, l < n_var), l, j, left),
            (l >= n_var, l - TWICE, left, right),
        ):

            @pl.when(here)
            def _():
                remote(back.at[l, rows(p), :], out.at[at, :, cols(quarter)], b_send, b_recv, member=p).start()
                out[at, :, cols(quarter)] = back[l, rows(j), :]

        @pl.when(l < n_var + TWICE - 1)
        def _():
            with jax.named_scope("gain"):
                anomalies_of(l + 1, 1 - slot)
                for w in range(3):
                    gain_of(1 - slot, w, (l + 1) // n_var)

        return c

    lax.fori_loop(0, n_var + TWICE, analyse, 0)

    with jax.named_scope("fin"):
        got = (3 * n_var - TWICE) * own
        deep = next(k for k in range(1, n_var) if got % (16 * k) == 0 and got // k <= peers * own)
        back_in = back.at[pl.ds(0, deep), pl.ds(0, got // deep), :]
        remote(back_in, back_in, b_send, b_recv, member=opp).wait_recv()

    with jax.named_scope("sent"):
        remote(back_in, back_in, b_send, b_recv, member=opp).wait_send()
        ens_in = recv.at[:, pl.ds(0, 3 * own), :]
        remote(ens_in, ens_in, e_send, e_recv.at[0], member=opp).wait_send()
        halves = obs.at[1, 0, pl.ds(0, 3 * own), :]
        remote(halves, halves, o_send, o_recv.at[0], member=opp).wait_send()
        remote(halves, halves, y_send, y_recv.at[0], depth=1 - d).wait_send()
        for k, p, has, seam in sides:

            @pl.when(has)
            def _():
                small_copy(k, after).wait_send()
                remote(obs.at[1], obs.at[2 * k], n_send.at[k], n_recv.at[0, k], region=after).wait_send()

        summed.wait_send()
        swap.wait_send()
        told(0).wait_send()
        told(1).wait_send()


def solution(mesh):
    regions, peers = mesh.shape["region"], mesh.shape["member"]

    def shards(ensemble, obs_weights, obs_tiles, obs_values, obs_error, obs_noise):
        n_var, own, n_tile = ensemble.shape
        n_obs = obs_tiles.shape[0]
        share, members = n_tile // peers, own * peers
        DMA = pltpu.SemaphoreType.DMA
        scratch = [
            pltpu.VMEM((n_var, own, n_tile), BF16),
            pltpu.SMEM((n_var,), F32),
            pltpu.VMEM((1, n_obs), jnp.int32),
            pltpu.VMEM((3, 8, n_obs), F32),
            pltpu.VMEM((own, n_obs), F32),
            pltpu.VMEM((2, own, n_obs), BF16),
            pltpu.VMEM((3, 2, members, n_obs), BF16),
            pltpu.VMEM((peers, 2, n_obs), F32),
            pltpu.VMEM((2, RING, 8, 128), F32),
            pltpu.VMEM((n_var + TWICE, members, share), BF16),
            pltpu.VMEM((n_var + TWICE, members, share), BF16),
            pltpu.VMEM((2, members, share), BF16),
            pltpu.VMEM((2, 8, share), F32),
            pltpu.VMEM((3 * n_obs, members), BF16),
            pltpu.VMEM((2, 3 * n_obs, share), F32),
            pltpu.VMEM((2, 3 * n_obs, share), BF16),
            pltpu.VMEM((members, 3 * n_obs), BF16),
            pltpu.VMEM((3, 8, n_obs), F32),
            DMA((7,)),
            DMA,
            DMA((n_var + 3 * TWICE,)),
            DMA,
            DMA,
            DMA,
            DMA((4,)),
            DMA,
            DMA((4,)),
            DMA((2,)),
            DMA((2, 2)),
            DMA((2,)),
            DMA((2,)),
            DMA,
            DMA,
            DMA,
            DMA,
            DMA((2,)),
            DMA((2,)),
        ]
        hbm = pl.BlockSpec(memory_space=pltpu.HBM)
        analysis, inflation = pl.pallas_call(
            lambda *refs: kernel(regions, peers, RING, *refs),
            out_shape=(
                pltpu.VMEM(ensemble.shape, BF16),
                pltpu.VMEM((1, 1), F32),
            ),
            in_specs=[hbm] * 6,
            out_specs=(pl.BlockSpec(memory_space=pltpu.VMEM), pl.BlockSpec(memory_space=pltpu.VMEM)),
            scratch_shapes=scratch,
            compiler_params=pltpu.CompilerParams(
                collective_id=0, has_side_effects=True, vmem_limit_bytes=56 * 2**20
            ),
        )(
            ensemble,
            obs_weights,
            obs_tiles.reshape(1, n_obs),
            obs_values.reshape(1, n_obs),
            obs_error.reshape(1, n_obs),
            obs_noise,
        )
        return analysis, inflation.reshape(())

    return jax.shard_map(
        shards,
        mesh=mesh,
        in_specs=(
            P("depth", "member", "region"),
            P("depth"),
            P("region"),
            P("region"),
            P("region"),
            P("member", "region"),
        ),
        out_specs=(P("depth", "member", "region"), P()),
        check_vma=False,
    )
```
